256 devices in a mesh: dp: 4 (over y_hi, core), seq: 64 (over z, x, y_lo).
Axes of the slice: x: 4, y: 4 (y_hi: 2, y_lo: 2; y = y_hi * 2 + y_lo), z: 8, core: 2. Of those that a mesh axis runs over, the one named last changes fastest.
Arguments:
- queries: bfloat16 [4, 8192, 2048], P('dp', 'seq'), may hold values from -12 to 12
- keys: bfloat16 [4, 8192, 512], P('dp', 'seq'), may hold values from -4 to 4
- values: bfloat16 [4, 8192, 512], P('dp', 'seq'), may hold values from -6 to 6
- segments: int32 [4, 8192], P('dp', 'seq'), may hold values from 0 to 3, never falling along the last dimension, each value on 1 to 7168 neighbouring positions
- task_ids: int32 [4], replicated, may hold values from 0 to 127
- prompt_keys: bfloat16 [128, 128, 512], P('seq'), may hold values from -4 to 4
- prompt_values: bfloat16 [128, 128, 512], P('seq'), may hold values from -6 to 6
- grad_out: bfloat16 [4, 8192, 2048], P('dp', 'seq'), may hold values from -6 to 6
Outputs:
- attended: bfloat16 [4, 8192, 2048], P('dp', 'seq')
- prompt_key_grad: float32 [128, 128, 512], P('seq')
- prompt_value_grad: float32 [128, 128, 512], P('seq')
The draws below stay inside these ranges and needn't reach their ends.
Inputs may be any that keep to these rules, and one draw needn't show every extreme that they name: `segments`: along each example the document numbers never fall; one document holds 7168 tokens.
All inputs are finite; a program needn't handle non-finite values.
Results may differ from the reference program's by a relative error of at most 0.0096.
Values may be sent and summed in bfloat16 or wider, within the bound.
No kernel may reach another device: no remote copies, remote signals or barrier semaphores. Data moves between devices by JAX's collectives and lax.ppermute only.
A program may use at most 128 MiB of HBM per device.

```python
import math
import jax
import jax.numpy as jnp
import numpy as np
from jax import lax

KVH = 4
GROUP = 4
HD = 128
PROMPT = 128
DOCS = 4
HEADS = 16
TOKENS = 8192
TASKS = 128
BATCH = 4
LONGEST = 7168


def draw_queries(key, part):
    base_key = jax.random.fold_in(key, 7)
    shape = (BATCH, TOKENS, KVH * GROUP * HD)
    field = jnp.clip(3.0 * jax.random.normal(base_key, shape, jnp.float32), -12.0, 12.0)
    return field.astype(jnp.bfloat16)


def draw_prompt_keys(key, part):
    base_key = jax.random.fold_in(key, 11)
    shape = (TASKS, PROMPT, KVH * HD)
    field = jnp.clip(jax.random.normal(base_key, shape, jnp.float32), -4.0, 4.0)
    return field.astype(jnp.bfloat16)


def with_ends(result, stream_key, smallest, top_value):
    longest = result.shape.index(max(result.shape))
    spots = []
    for shift in (0, 1):
        where = [jax.random.randint(jax.random.fold_in(stream_key, axis), (), 0, length) for axis, length in enumerate(result.shape)]
        where[longest] = (where[longest] + shift) % result.shape[longest]
        spots.append(tuple(where))
    return result.at[spots[0]].set(smallest).at[spots[1]].set(top_value)


def block_levels(key, extent, shards, least, high):
    level = 1.0
    for dim, shards_of in shards:
        draws = jax.random.uniform(jax.random.fold_in(jax.random.fold_in(key, 6), dim), (shards_of,), jnp.float32, least / len(shards), high / len(shards))
        level = level * jnp.repeat(jnp.exp(draws), extent[dim] // shards_of).reshape((-1,) + (1,) * (len(extent) - 1 - dim))
    return level


def split_up(count, total, bound, skew):
    weights = [(1 << 20) // math.isqrt(rank ** skew) + 1 for rank in range(2, count + 1)]
    spare, given = total - bound - (count - 1), [1] * (count - 1)
    while spare > 0:
        candidates = [i for i in range(count - 1) if given[i] < bound]
        mass, left = sum([weights[i] for i in candidates]), spare
        for i in candidates:
            more = min(bound - given[i], max(1, left * weights[i] // mass), spare)
            given[i] = given[i] + more
            spare = spare - more
    return np.array([bound] + given)


def uneven_parts(key, number_of, total, limit, skew):
    if number_of == 2:
        one = jax.random.randint(key, (), max(1, total - limit), min(limit, total - 1) + 1)
        return jnp.stack([one, total - one])
    lengths = jnp.asarray(split_up(number_of, total, limit, skew), jnp.int32)
    couples = (number_of - 1) // 2
    giver, taker = lengths[1:1 + 2 * couples:2], lengths[2:2 + 2 * couples:2]
    slack = jnp.minimum(giver - 1, limit - taker)
    moved = jax.random.randint(jax.random.fold_in(key, 1), (couples,), 0, 1 << 20) % (slack + 1)
    lengths = lengths.at[1:1 + 2 * couples:2].set(giver - moved).at[2:2 + 2 * couples:2].set(taker + moved)
    return lengths[jax.random.permutation(jax.random.fold_in(key, 2), number_of)]


def noise(own_key, shape, width, most, shards=(), kind=jnp.bfloat16):
    result = jax.random.normal(own_key, shape, jnp.float32) * width
    if len(shards) > 0:
        result = block_levels(own_key, shape, shards, -0.22, 0.18) * result
    return jnp.clip(result, min=-most, max=most).astype(kind)


def setup_inputs(seed: int = 0) -> dict:
    arg_keys = jax.random.split(jax.random.key(seed), 9)
    queries = draw_queries(jax.random.fold_in(arg_keys[8], 71), 0)
    keys = noise(arg_keys[1], (BATCH, TOKENS, KVH * HD), 1.0, 4.0, ((0, 4), (1, 64)))
    values = noise(arg_keys[2], (BATCH, TOKENS, KVH * HD), 1.0, 6.0, ((0, 4), (1, 64)))
    segments = jax.vmap(lambda own: jnp.searchsorted(jnp.cumsum(uneven_parts(own, DOCS, TOKENS, LONGEST, 2)), jnp.arange(TOKENS), side="right"))(jax.random.split(arg_keys[3], BATCH)).reshape((BATCH, TOKENS)).astype(jnp.int32)
    task_ids = with_ends(jax.random.randint(arg_keys[4], (BATCH,), 0, TASKS), jax.random.fold_in(arg_keys[4], 1), 0, TASKS - 1).astype(jnp.int32)
    prompt_keys = draw_prompt_keys(jax.random.fold_in(arg_keys[8], 71), 0)
    prompt_values = noise(arg_keys[6], (TASKS, PROMPT, KVH * HD), 1.0, 6.0, ((0, 64),))
    grad_out = noise(arg_keys[7], (BATCH, TOKENS, HEADS * HD), 1.0, 6.0, ((0, 4), (1, 64)))
    return dict(queries=queries, keys=keys, values=values, segments=segments, task_ids=task_ids, prompt_keys=prompt_keys, prompt_values=prompt_values, grad_out=grad_out)


def rounded(tensor):
    return lax.optimization_barrier(tensor.astype(jnp.bfloat16)).astype(jnp.float32)

def one_example(query_rows, key_rows, value_rows, segment_row, grad_rows, chosen_keys, chosen_values):
    tokens_all = query_rows.shape[0]
    block_rows = math.gcd(tokens_all, 256)
    block_count = tokens_all // block_rows
    scaling = 1.0 / math.sqrt(HD)
    key_heads = key_rows.reshape(tokens_all, KVH, HD).astype(jnp.float32)
    value_heads = value_rows.reshape(tokens_all, KVH, HD).astype(jnp.float32)
    prompt_key_heads = chosen_keys.reshape(PROMPT, KVH, HD).astype(jnp.float32)
    prompt_value_heads = chosen_values.reshape(PROMPT, KVH, HD).astype(jnp.float32)
    key_index = lax.iota(jnp.int32, tokens_all)

    def per_block(carried, block_index):
        first_row = (block_index * block_rows).astype(jnp.int32)
        query_heads = lax.dynamic_slice_in_dim(query_rows, first_row, block_rows, 0)
        query_heads = query_heads.reshape(block_rows, KVH, GROUP, HD).astype(jnp.float32)
        grad_heads = lax.dynamic_slice_in_dim(grad_rows, first_row, block_rows, 0)
        grad_heads = grad_heads.reshape(block_rows, KVH, GROUP, HD).astype(jnp.float32)
        query_segments = lax.dynamic_slice_in_dim(segment_row, first_row, block_rows, 0)
        query_index = first_row + lax.iota(jnp.int32, block_rows)
        visible = (segment_row[None, :] == query_segments[:, None]) & (key_index[None, :] <= query_index[:, None])
        mask_wide = visible[:, None, None, :]
        scores = jnp.einsum('tkgd,skd->tkgs', query_heads, key_heads) * scaling
        prompt_scores = jnp.einsum('tkgd,pkd->tkgp', query_heads, prompt_key_heads) * scaling
        new_peak = jnp.maximum(lax.optimization_barrier(jnp.max(jnp.where(mask_wide, scores, -jnp.inf), axis=-1)), lax.optimization_barrier(jnp.max(prompt_scores, axis=-1)))
        weights = jnp.where(mask_wide, jnp.exp(scores - new_peak[..., None]), 0.0)
        prompt_weights = jnp.exp(prompt_scores - new_peak[..., None])
        totals = lax.optimization_barrier(jnp.sum(weights, axis=-1)) + lax.optimization_barrier(jnp.sum(prompt_weights, axis=-1))
        accumulated = jnp.einsum('tkgs,skd->tkgd', rounded(weights), value_heads)
        accumulated = accumulated + jnp.einsum('tkgp,pkd->tkgd', rounded(prompt_weights), prompt_value_heads)
        attended = (accumulated / totals[..., None]).astype(jnp.bfloat16)
        log_norm = new_peak + jnp.log(totals)
        attended_wide = lax.optimization_barrier(attended).astype(jnp.float32)
        row_delta = lax.optimization_barrier(jnp.sum(grad_heads * attended_wide, axis=-1))
        prompt_probs = jnp.exp(prompt_scores - log_norm[..., None])
        prompt_dots = jnp.einsum('tkgd,pkd->tkgp', grad_heads, prompt_value_heads)
        score_grad = prompt_probs * (prompt_dots - row_delta[..., None])
        value_part = jnp.einsum('tkgp,tkgd->pkd', rounded(prompt_probs), grad_heads)
        key_part = jnp.einsum('tkgp,tkgd->pkd', rounded(score_grad), query_heads) * scaling
        return ((carried[0] + key_part, carried[1] + value_part), attended.reshape(block_rows, KVH * GROUP * HD))
    zeros = jnp.zeros((PROMPT, KVH, HD), jnp.float32)
    sums, pieces = lax.scan(per_block, (zeros, zeros), jnp.arange(block_count, dtype=jnp.int32))
    attended_all = pieces.reshape(tokens_all, KVH * GROUP * HD)
    return (attended_all, sums[0].reshape(PROMPT, KVH * HD), sums[1].reshape(PROMPT, KVH * HD))

def reference(queries, keys, values, segments, task_ids, prompt_keys, prompt_values, grad_out):
    outputs = []
    key_grad = jnp.zeros((TASKS, PROMPT, KVH * HD), jnp.float32)
    value_grad = jnp.zeros((TASKS, PROMPT, KVH * HD), jnp.float32)
    task_range = lax.iota(jnp.int32, TASKS)
    for example in range(queries.shape[0]):
        task_now = task_ids[example].astype(jnp.int32)
        chosen_keys = lax.dynamic_index_in_dim(prompt_keys, task_now, 0, keepdims=False)
        chosen_values = lax.dynamic_index_in_dim(prompt_values, task_now, 0, keepdims=False)
        attended, key_part, value_part = one_example(queries[example], keys[example], values[example], segments[example], grad_out[example], chosen_keys, chosen_values)
        outputs.append(attended)
        chosen = (task_range == task_now)[:, None, None]
        key_grad = key_grad + jnp.where(chosen, key_part[None], 0.0)
        value_grad = value_grad + jnp.where(chosen, value_part[None], 0.0)
    return (jnp.stack(outputs), key_grad, value_grad)
```

```python
import math

import jax
import jax.numpy as jnp
from jax import lax
from jax.experimental import pallas as pl
from jax.experimental.pallas import tpu as pltpu
from jax.sharding import Mesh
from jax.sharding import PartitionSpec as P

KVH = 4
GROUP = 4
HD = 128
PROMPT = 128
TOK = 128
CHUNK = 272
SEQ = ("zh", "zl", "x", "y")
ALL = ("dp", "zh", "zl", "x", "y")
SCALE = 1.0 / math.sqrt(HD)
LOG2E = math.log2(math.e)
HIDDEN = -1e30


ORDER = [(a, b, c) for c in (0, -1, 1, 2) for a in (0, 1) for b in (0, 1)]


def dot_nt(a, b):
    return lax.dot_general(a, b, (((1,), (1,)), ((), ())), preferred_element_type=jnp.float32)


def dot_tn(a, b):
    return lax.dot_general(a, b, (((0,), (0,)), ((), ())), preferred_element_type=jnp.float32)


def dot_nn(a, b):
    return lax.dot_general(a, b, (((1,), (0,)), ((), ())), preferred_element_type=jnp.float32)


def stacked_heads(block):
    return jnp.concatenate([block[:, g * HD : (g + 1) * HD] for g in range(GROUP)], axis=0)


def attention_kernel(before_ref, q_ref, go_ref, prompt_ref, *rest):
    chunks = rest[:16]
    att_ref, grads_ref, acc_ref, peak_ref = rest[16:]
    factor = SCALE * LOG2E
    prompt_k = jnp.concatenate([prompt_ref[:, 0:HD], prompt_ref[:, HD : 2 * HD]], axis=0)
    prompt_v = jnp.concatenate([prompt_ref[:, 2 * HD : 3 * HD], prompt_ref[:, 3 * HD :]], axis=0)
    ones_p = jnp.ones((PROMPT, HD), jnp.bfloat16)
    grads_ref[...] = jnp.zeros_like(grads_ref)

    def per_block(k, _):
        q = stacked_heads(q_ref[k])
        own_seg = chunks[0][k, 2 * TOK : 2 * TOK + 16, :].astype(jnp.float32)[0:1]
        seg_q = jnp.transpose(jnp.broadcast_to(own_seg, (TOK, TOK)))
        scores = dot_nt(q, prompt_k)
        peak = jnp.max(scores, axis=1, keepdims=True)
        weights = jnp.exp2((scores - peak) * factor)
        acc_ref[...] = dot_nn(
            weights.astype(jnp.bfloat16), jnp.concatenate([prompt_v, ones_p], axis=1)
        )
        peak_ref[...] = peak

        def absorb(j, some, diagonal):
            keys = jnp.concatenate([chunks[n][j, 0:TOK, :] for n in some], axis=0)
            values = jnp.concatenate([chunks[n][j, TOK : 2 * TOK, :] for n in some], axis=0)
            count = len(some) * TOK
            visible = []
            for n in some:
                seg = chunks[n][j, 2 * TOK : 2 * TOK + 16, :].astype(jnp.float32)[0:1]
                if diagonal and n != 0:
                    seg = jnp.where(before_ref[n] > 0, seg, -1.0)
                same = seg_q == seg
                if diagonal and n == 0:
                    rows = lax.broadcasted_iota(jnp.int32, (TOK, TOK), 0)
                    cols = lax.broadcasted_iota(jnp.int32, (TOK, TOK), 1)
                    same = same & (cols <= rows)
                visible.append(same)
            visible = jnp.concatenate(visible, axis=1)
            scores = dot_nt(q, keys).reshape(GROUP, TOK, count)
            scores = jnp.where(visible[None], scores, HIDDEN).reshape(GROUP * TOK, count)
            old = peak_ref[...]
            peak = jnp.maximum(old, jnp.max(scores, axis=1, keepdims=True))
            weights = jnp.exp2((scores - peak) * factor)
            shrink = jnp.exp2((old - peak) * factor)
            wide = jnp.concatenate([values, jnp.ones((count, HD), jnp.bfloat16)], axis=1)
            acc_ref[...] = acc_ref[...] * shrink + dot_nn(weights.astype(jnp.bfloat16), wide)
            peak_ref[...] = peak

        def earlier(j, _):
            absorb(j, range(0, 8), False)
            absorb(j, range(8, 16), False)
            return 0

        lax.fori_loop(0, k, earlier, 0)
        absorb(k, range(0, 8), True)
        absorb(k, range(8, 16), True)
        norm = acc_ref[:, HD:]
        attended = (acc_ref[:, :HD] / norm).astype(jnp.bfloat16)
        for g in range(GROUP):
            att_ref[k, :, g * HD : (g + 1) * HD] = attended[g * TOK : (g + 1) * TOK]
        go = stacked_heads(go_ref[k])
        delta = jnp.sum(
            go.astype(jnp.float32) * attended.astype(jnp.float32), axis=1, keepdims=True
        )
        log_norm = peak_ref[...] * factor + jnp.log2(norm)
        probs = jnp.exp2(dot_nt(q, prompt_k) * factor - log_norm)
        score_grad = probs * (dot_nt(go, prompt_v) - delta)
        grads_ref[0:PROMPT, :] += dot_tn(score_grad.astype(jnp.bfloat16), q) * SCALE
        grads_ref[PROMPT:, :] += dot_tn(probs.astype(jnp.bfloat16), go)
        return 0

    lax.fori_loop(0, KVH, per_block, 0)


def attend(before, q, go, prompt, chunks):
    vmem = pl.BlockSpec(memory_space=pltpu.VMEM)
    return pl.pallas_call(
        attention_kernel,
        out_shape=(
            jax.ShapeDtypeStruct((KVH, TOK, GROUP * HD), jnp.bfloat16),
            jax.ShapeDtypeStruct((2 * PROMPT, HD), jnp.float32),
        ),
        in_specs=[pl.BlockSpec(memory_space=pltpu.SMEM)] + [vmem] * (3 + 16),
        out_specs=(vmem, vmem),
        scratch_shapes=[
            pltpu.VMEM((GROUP * TOK, 2 * HD), jnp.float32),
            pltpu.VMEM((GROUP * TOK, 1), jnp.float32),
        ],
        compiler_params=pltpu.CompilerParams(vmem_limit_bytes=48 * 1024 * 1024),
        name="attend",
    )(before, q, go, prompt, *chunks)


def swap(value, axis):
    return lax.ppermute(value, axis, [(0, 1), (1, 0)])


def from_left(value):
    return lax.ppermute(value, "x", [(i, (i + 1) % 4) for i in range(4)])


def from_right(value):
    return lax.ppermute(value, "x", [(i, (i - 1) % 4) for i in range(4)])


def exchange(blocks):
    return lax.all_to_all(blocks, "zh", 0, 0, tiled=True)


def gather_chunks(own):
    got = {(0, 0, 0): own}
    got[1, 0, 0] = swap(own, "zl")
    got[0, 1, 0] = swap(own, "y")
    got[0, 0, -1] = from_left(own)
    got[0, 0, 1] = from_right(own)
    got[1, 0, -1] = from_left(got[1, 0, 0])
    got[1, 0, 1] = from_right(got[1, 0, 0])
    got[0, 1, -1] = from_left(got[0, 1, 0])
    got[0, 1, 1] = from_right(got[0, 1, 0])
    got[1, 1, 0] = swap(got[1, 0, 0], "y")
    got[0, 0, 2] = from_left(got[0, 0, -1])
    got[1, 0, 2] = from_right(got[1, 0, 1])
    got[1, 1, -1] = swap(got[1, 0, -1], "y")
    got[1, 1, 1] = swap(got[0, 1, 1], "zl")
    got[0, 1, 2] = swap(got[0, 0, 2], "y")
    got[1, 1, 2] = swap(got[1, 0, 2], "y")
    return [got[key] for key in ORDER]


def choose(index, mine, own, others):
    chosen = own
    for position, other in others:
        chosen = jnp.where(index == position, other, chosen)
    return chosen


def shards(queries, keys, values, segments, task_ids, prompt_keys, prompt_values, grad_out):
    dp, zh, zl, x, y = (lax.axis_index(name) for name in ALL)
    seq_rank = ((zh * 2 + zl) * 4 + x) * 2 + y
    my_task = task_ids[dp]
    owner, slot = my_task // 2, my_task % 2
    own_zh, own_zl, own_x, own_y = owner // 16, (owner // 8) % 2, (owner // 2) % 4, owner % 2

    def by_head(rows, width):
        return rows.reshape(TOK, KVH, width).transpose(1, 0, 2)

    seg_rows = jnp.broadcast_to(
        segments.astype(jnp.bfloat16)[:, None], (KVH, CHUNK - 2 * TOK, TOK)
    )
    payload = jnp.concatenate([by_head(keys[0], HD), by_head(values[0], HD), seg_rows], axis=1)
    chunks = gather_chunks(exchange(payload))

    offsets = []
    for a, b, c in ORDER:
        offsets.append((zl + a) % 2 * 8 + (x + c) % 4 * 2 + (y + b) % 2)
    offsets = jnp.stack(offsets)
    before = (offsets < offsets[0]).astype(jnp.int32)

    q = exchange(by_head(queries[0], GROUP * HD))
    pair = jnp.stack(
        [
            lax.dynamic_index_in_dim(prompt_keys, slot, 0, keepdims=False),
            lax.dynamic_index_in_dim(prompt_values, slot, 0, keepdims=False),
        ]
    )
    pair = pair.reshape(2, 2, 64, KVH, HD).transpose(3, 2, 0, 1, 4).reshape(KVH, 64, 4 * HD)
    both = exchange(jnp.concatenate([by_head(grad_out[0], GROUP * HD), pair], axis=1))
    go = both[:, :TOK]
    prompt = lax.dynamic_index_in_dim(both, own_zh, 0, keepdims=False)[TOK:]
    prompt = choose(own_zl, zl, prompt, [(1 - zl, swap(prompt, "zl"))])
    prompt = choose(own_y, y, prompt, [(1 - y, swap(prompt, "y"))])
    left, right = from_left(prompt), from_right(prompt)
    across = lax.ppermute(prompt, "x", [(i, (i + 2) % 4) for i in range(4)])
    prompt = choose(
        own_x, x, prompt, [((x + 3) % 4, left), ((x + 1) % 4, right), ((x + 2) % 4, across)]
    )

    attended, grads = attend(before, q, go, prompt, chunks)
    attended = exchange(attended).transpose(1, 0, 2).reshape(1, TOK, KVH * GROUP * HD)

    pieces = grads.astype(jnp.bfloat16).reshape(16, 16, HD)
    pieces = lax.all_to_all(pieces, ("zl", "x", "y"), 0, 0, tiled=True)
    piece = jnp.sum(pieces.astype(jnp.float32), axis=0).astype(jnp.bfloat16)
    sent = jnp.broadcast_to(piece[None], (256, 16, HD))
    sent = lax.all_to_all(sent, ALL, 0, 0, tiled=True)
    whole = sent.reshape(4, KVH, 2, PROMPT, HD)
    own_tasks = seq_rank * 2 + lax.iota(jnp.int32, 2)
    matches = (task_ids[:, None] == own_tasks[None, :])[:, :, None, None, None]

    def bank(part):
        total = jnp.sum(jnp.where(matches, part[:, None].astype(jnp.float32), 0.0), axis=0)
        return total.transpose(0, 2, 1, 3).reshape(2, PROMPT, KVH * HD)

    return attended, bank(whole[:, :, 0]), bank(whole[:, :, 1])


def solution(mesh):
    split = Mesh(mesh.devices.reshape(4, 4, 2, 4, 2), ALL)
    return jax.shard_map(
        shards,
        mesh=split,
        in_specs=(
            P("dp", SEQ, None),
            P("dp", SEQ, None),
            P("dp", SEQ, None),
            P("dp", SEQ),
            P(),
            P(SEQ, None, None),
            P(SEQ, None, None),
            P("dp", SEQ, None),
        ),
        out_specs=(P("dp", SEQ, None), P(SEQ, None, None), P(SEQ, None, None)),
        check_vma=False,
    )
```

```python
import math

import jax
import jax.numpy as jnp
from jax import lax
from jax.experimental import pallas as pl
from jax.experimental.pallas import tpu as pltpu
from jax.sharding import Mesh
from jax.sharding import PartitionSpec as P

KVH = 4
GROUP = 4
HD = 128
PROMPT = 128
TOK = 128
WIDE = GROUP * HD
ZS = 8
CHUNK = 272
SEQ = ("zh", "zl", "x", "y")
ALL = ("dp", "zh", "zl", "x", "y")
SCALE = 1.0 / math.sqrt(HD)
LOG2E = math.log2(math.e)
FACTOR = SCALE * LOG2E
HIDDEN = -1e30
SPLIT = 2


ORDER = [(0, 0), (1, 0), (0, -1), (0, 1), (0, 2), (1, -1), (1, 1), (1, 2)]

VMEM = pl.BlockSpec(memory_space=pltpu.VMEM)
SMEM = pl.BlockSpec(memory_space=pltpu.SMEM)


HBM = pl.BlockSpec(memory_space=pltpu.HBM)


def params(mib=24):
    return pltpu.CompilerParams(vmem_limit_bytes=mib * 1024 * 1024)


def dot_nt(a, b):
    return lax.dot_general(a, b, (((1,), (1,)), ((), ())), preferred_element_type=jnp.float32)


def dot_tn(a, b):
    return lax.dot_general(a, b, (((0,), (0,)), ((), ())), preferred_element_type=jnp.float32)


def dot_nn(a, b):
    return lax.dot_general(a, b, (((1,), (0,)), ((), ())), preferred_element_type=jnp.float32)


def stacked_heads(block):
    return jnp.concatenate([block[:, g * HD : (g + 1) * HD] for g in range(GROUP)], axis=0)


def keys_kernel(keys_ref, values_ref, segments_ref, out_ref, seg_ref, sems):
    copies = [pltpu.make_async_copy(segments_ref, seg_ref, sems.at[0])]
    for z in range(ZS):
        cols = pl.ds(z // 2 * HD, HD)
        for n, source in enumerate((keys_ref, values_ref)):
            target = out_ref.at[z, pl.ds(n * TOK, TOK), :]
            copies.append(
                pltpu.make_async_copy(source.at[0, :, cols], target, sems.at[1 + 2 * z + n])
            )
    for copy in copies:
        copy.start()
    copies[0].wait()
    seg = seg_ref[...].astype(jnp.float32).astype(jnp.bfloat16)
    for z in range(ZS):
        out_ref[z, 2 * TOK : CHUNK, :] = jnp.broadcast_to(seg, (CHUNK - 2 * TOK, TOK))
    for copy in copies[1:]:
        copy.wait()


def keys_payload(keys, values, segments):
    return pl.pallas_call(
        keys_kernel,
        out_shape=jax.ShapeDtypeStruct((ZS, CHUNK, HD), jnp.bfloat16),
        in_specs=[HBM, HBM, HBM],
        out_specs=VMEM,
        scratch_shapes=[
            pltpu.VMEM((1, TOK), jnp.int32),
            pltpu.SemaphoreType.DMA((1 + 2 * ZS,)),
        ],
        compiler_params=params(),
        name="keys_payload",
    )(keys, values, segments)


def rows_kernel(tasks_ref, queries_ref, go_ref, pk_ref, pv_ref, *rest):
    outs, sems = rest[: 3 * KVH], rest[3 * KVH]
    slot = tasks_ref[lax.axis_index("dp")] % 2
    zh = lax.axis_index("zh")
    half = PROMPT // 2
    copies = []

    def add(source, target):
        copies.append(pltpu.make_async_copy(source, target, sems.at[len(copies)]))

    for d in range(KVH):
        h = (zh + d) % KVH
        cols = pl.ds(pl.multiple_of(h * WIDE, WIDE), WIDE)
        q_out, go_out, prompt_out = outs[d], outs[KVH + d], outs[2 * KVH + d]
        add(queries_ref.at[0, :, cols], q_out)
        own = pl.ds(pl.multiple_of(h * HD, HD), HD)
        for n, bank in enumerate((pk_ref, pv_ref)):
            for s in range(2):
                place = pl.ds((2 * n + s) * HD, HD)
                add(
                    bank.at[slot, pl.ds(s * half, half), own],
                    prompt_out.at[:, place],
                )
        add(go_ref.at[0, :, cols], go_out)
    for copy in copies:
        copy.start()
    for copy in copies:
        copy.wait()


def rows_payload(tasks, queries, go, prompt_keys, prompt_values):
    outs = pl.pallas_call(
        rows_kernel,
        out_shape=[jax.ShapeDtypeStruct((TOK, WIDE), jnp.bfloat16)] * (2 * KVH)
        + [jax.ShapeDtypeStruct((PROMPT // 2, WIDE), jnp.bfloat16)] * KVH,
        in_specs=[SMEM, HBM, HBM, HBM, HBM],
        out_specs=[VMEM] * (3 * KVH),
        scratch_shapes=[pltpu.SemaphoreType.DMA((6 * KVH,))],
        compiler_params=params(),
        name="rows_payload",
    )(tasks, queries, go, prompt_keys, prompt_values)
    return outs[:KVH], outs[KVH : 2 * KVH], outs[2 * KVH :]


class Bundle:
    def __init__(self, ref):
        self.ref = ref

    def keys(self, z):
        return self.ref[z, 0:TOK, :]

    def values(self, z):
        return self.ref[z, TOK : 2 * TOK, :]

    def segments(self, z):
        return self.ref[z, 2 * TOK : CHUNK, :].astype(jnp.float32)[0:1]


def accumulate(scores, wide, acc_ref, peak_ref, rows):
    old = peak_ref[rows]
    peak = jnp.maximum(old, jnp.max(scores, axis=1, keepdims=True))
    weights = jnp.exp2((scores - peak) * FACTOR).astype(jnp.bfloat16)
    shrink = jnp.exp2((old - peak) * FACTOR)
    acc_ref[rows] = acc_ref[rows] * shrink + dot_nn(weights, wide)
    peak_ref[rows] = peak


def absorb(bundles, j, q, seg_q, diagonal, acc_ref, peak_ref):
    zl, x, y = (lax.axis_index(name) for name in ("zl", "x", "y"))
    count = len(bundles) * 2 * TOK
    keys, values, visible = [], [], []
    for e in range(2):
        z = 2 * j + e
        for n, part in bundles.items():
            keys.append(part.keys(z))
            values.append(part.values(z))
            seg = part.segments(z)
            if diagonal and n != 0:
                b, c = ORDER[n]
                before = ((x + c + 4) % 4 * 2 + (y + b) % 2) < x * 2 + y
                shown = (zl > e) | ((zl == e) & before)
                seg = jnp.where(shown, seg, -1.0)
            same = seg_q == seg
            if diagonal and n == 0:
                reach = jnp.where(zl == e, 0, jnp.where(zl > e, TOK, -TOK))
                rows = lax.broadcasted_iota(jnp.int32, (TOK, TOK), 0)
                cols = lax.broadcasted_iota(jnp.int32, (TOK, TOK), 1)
                same = same & (cols - rows <= reach)
            visible.append(same)
    keys = jnp.concatenate(keys, axis=0)
    values = jnp.concatenate(values, axis=0)
    visible = jnp.concatenate(visible, axis=1)[None]
    wide = jnp.concatenate([values, jnp.ones(values.shape, jnp.bfloat16)], axis=1)
    size = GROUP * TOK // SPLIT
    scores = []
    for g in range(SPLIT):
        part = dot_nt(q[g * size : (g + 1) * size], keys).reshape(size // TOK, TOK, count)
        scores.append(jnp.where(visible, part, HIDDEN).reshape(size, count))
    for g in range(SPLIT):
        rows = slice(g * size, (g + 1) * size)
        accumulate(scores[g], wide, acc_ref, peak_ref, rows)


def sweep(bundles, own_ref, q, k, acc_ref, peak_ref):
    seg = own_ref[2 * k + lax.axis_index("zl"), 2 * TOK :, :].astype(jnp.float32)[0:1]
    seg_q = jnp.transpose(jnp.broadcast_to(seg, (TOK, TOK)))
    absorb(bundles, k, q, seg_q, True, acc_ref, peak_ref)

    def earlier(j, carry):
        absorb(bundles, j, q, seg_q, False, acc_ref, peak_ref)
        return carry

    lax.fori_loop(0, k, earlier, 0)


def first_kernel(names, *refs):
    q_refs, refs = refs[:KVH], refs[KVH:]
    bundles = {n: Bundle(ref) for n, ref in zip(names, refs)}
    refs = refs[len(names) :]
    out_ref, q_ref, state_ref, acc_ref, peak_ref, sems = refs
    own_ref = bundles[0].ref
    zh = lax.axis_index("zh")
    for d in range(KVH):
        q_ref[d] = stacked_heads(q_refs[d][...])

    def saved(d):
        return pltpu.make_async_copy(state_ref.at[d], out_ref.at[d], sems.at[d])

    def per_block(d, carry):
        acc_ref[...] = jnp.zeros_like(acc_ref)
        peak_ref[...] = jnp.full_like(peak_ref, HIDDEN)
        sweep(bundles, own_ref, q_ref[d], (zh - d + KVH) % KVH, acc_ref, peak_ref)
        state_ref[d, :, :HD] = acc_ref[:, :HD]
        lanes = lax.broadcasted_iota(jnp.int32, (GROUP * TOK, HD), 1)
        state_ref[d, :, HD:] = jnp.where(lanes < HD // 2, acc_ref[:, HD:], peak_ref[...])
        saved(d).start()
        return carry

    lax.fori_loop(0, KVH, per_block, 0)
    for d in range(KVH):
        saved(d).wait()


STATE = (KVH, GROUP * TOK, 2 * HD)


def cost(count):
    work = GROUP * TOK * HD * 4 * count * 2 * TOK * 10
    return pl.CostEstimate(flops=work, transcendentals=work // 512, bytes_accessed=1 << 22)


def attend_first(names, q, arrays):
    return pl.pallas_call(
        lambda *refs: first_kernel(names, *refs),
        out_shape=jax.ShapeDtypeStruct(STATE, jnp.float32),
        in_specs=[VMEM] * (KVH + len(arrays)),
        out_specs=pl.BlockSpec(memory_space=pltpu.HBM),
        scratch_shapes=[
            pltpu.VMEM((KVH, GROUP * TOK, HD), jnp.bfloat16),
            pltpu.VMEM(STATE, jnp.float32),
            pltpu.VMEM((GROUP * TOK, 2 * HD), jnp.float32),
            pltpu.VMEM((GROUP * TOK, 1), jnp.float32),
            pltpu.SemaphoreType.DMA((KVH,)),
        ],
        compiler_params=params(),
        cost_estimate=cost(len(names)),
        name="attend_first",
    )(*q, *arrays)


def last_kernel(names, *refs):
    q_refs, go_refs, refs = refs[:KVH], refs[KVH : 2 * KVH], refs[2 * KVH :]
    in_ref, own_ref, prompt_ref, *refs = refs
    bundles = {n: Bundle(ref) for n, ref in zip(names, refs)}
    refs = refs[len(names) :]
    att_refs, refs = refs[:KVH], refs[KVH:]
    grads_ref, q_ref, go_ref, state_ref, acc_ref, peak_ref, sums_ref, sems = refs
    zh = lax.axis_index("zh")

    def loaded(d):
        return pltpu.make_async_copy(in_ref.at[d], state_ref.at[d], sems.at[d])

    for d in range(KVH):
        loaded(d).start()
    for d in range(KVH):
        q_ref[d] = stacked_heads(q_refs[d][...])
        go_ref[d] = stacked_heads(go_refs[d][...])
    prompt_k = jnp.concatenate([prompt_ref[:, 0:HD], prompt_ref[:, HD : 2 * HD]], axis=0)
    prompt_v = jnp.concatenate([prompt_ref[:, 2 * HD : 3 * HD], prompt_ref[:, 3 * HD :]], axis=0)
    ones = jnp.ones(prompt_v.shape, jnp.bfloat16)
    prompt_wide = jnp.concatenate([prompt_v, ones], axis=1)
    sums_ref[...] = jnp.zeros_like(sums_ref)

    def per_block(d, carry):
        loaded(d).wait()
        q = q_ref[d]
        acc_ref[:, :HD] = state_ref[d, :, :HD]
        acc_ref[:, HD:] = jnp.broadcast_to(state_ref[d, :, HD : HD + 1], (GROUP * TOK, HD))
        peak_ref[...] = state_ref[d, :, 2 * HD - 1 :]
        accumulate(dot_nt(q, prompt_k), prompt_wide, acc_ref, peak_ref, slice(None))
        sweep(bundles, own_ref, q, (zh - d + KVH) % KVH, acc_ref, peak_ref)
        norm = acc_ref[:, HD:]
        attended = (acc_ref[:, :HD] / norm).astype(jnp.bfloat16)
        for n in range(KVH):

            @pl.when(d == n)
            def _():
                for g in range(GROUP):
                    att_refs[n][:, g * HD : (g + 1) * HD] = attended[g * TOK : (g + 1) * TOK]

        go = go_ref[d]
        delta = jnp.sum(
            go.astype(jnp.float32) * attended.astype(jnp.float32), axis=1, keepdims=True
        )
        log_norm = peak_ref[...] * FACTOR + jnp.log2(norm)
        probs = jnp.exp2(dot_nt(q, prompt_k) * FACTOR - log_norm)
        score_grad = probs * (dot_nt(go, prompt_v) - delta)
        sums_ref[0:PROMPT, :] += dot_tn(score_grad.astype(jnp.bfloat16), q) * SCALE
        sums_ref[PROMPT:, :] += dot_tn(probs.astype(jnp.bfloat16), go)
        return carry

    lax.fori_loop(0, KVH, per_block, 0)
    grads_ref[...] = sums_ref[...].astype(jnp.bfloat16)


def attend_last(names, q, go, state, own, prompt, arrays):
    outs = pl.pallas_call(
        lambda *refs: last_kernel(names, *refs),
        out_shape=[jax.ShapeDtypeStruct((TOK, WIDE), jnp.bfloat16)] * KVH
        + [jax.ShapeDtypeStruct((2 * PROMPT, HD), jnp.bfloat16)],
        in_specs=[VMEM] * (2 * KVH)
        + [pl.BlockSpec(memory_space=pltpu.HBM)]
        + [VMEM] * (2 + len(arrays)),
        out_specs=[VMEM] * (KVH + 1),
        scratch_shapes=[
            pltpu.VMEM((KVH, GROUP * TOK, HD), jnp.bfloat16),
            pltpu.VMEM((KVH, GROUP * TOK, HD), jnp.bfloat16),
            pltpu.VMEM(STATE, jnp.float32),
            pltpu.VMEM((GROUP * TOK, 2 * HD), jnp.float32),
            pltpu.VMEM((GROUP * TOK, 1), jnp.float32),
            pltpu.VMEM((2 * PROMPT, HD), jnp.float32),
            pltpu.SemaphoreType.DMA((KVH,)),
        ],
        compiler_params=params(),
        cost_estimate=cost(len(names) + 1),
        name="attend_last",
    )(*q, *go, state, own, prompt, *arrays)
    return outs[:KVH], outs[KVH]


def sum_kernel(pieces_ref, out_ref):
    total = pieces_ref[0].astype(jnp.float32)
    for r in range(1, 8):
        total += pieces_ref[r].astype(jnp.float32)
    for r in range(8):
        out_ref[r] = total.astype(jnp.bfloat16)


def summed(pieces):
    return pl.pallas_call(
        sum_kernel,
        out_shape=jax.ShapeDtypeStruct((8, 32, HD), jnp.bfloat16),
        in_specs=[VMEM],
        out_specs=VMEM,
        compiler_params=params(),
        name="summed",
    )(pieces)


def pairs_kernel(sent_ref, out_ref):
    for h in range(KVH):
        total = sent_ref[2 * h].astype(jnp.float32) + sent_ref[2 * h + 1].astype(jnp.float32)
        out_ref[h] = total.astype(jnp.bfloat16)


def pairs_summed(sent):
    return pl.pallas_call(
        pairs_kernel,
        out_shape=jax.ShapeDtypeStruct((KVH, 32, HD), jnp.bfloat16),
        in_specs=[VMEM],
        out_specs=VMEM,
        compiler_params=params(),
        name="pairs_summed",
    )(sent)


def route_kernel(tasks_ref, *refs):
    parts, out_ref = refs[:4], refs[4]
    dp = lax.axis_index("dp")
    first = (lax.axis_index("zh") * 2 + lax.axis_index("zl")) * 16
    tasks = [tasks_ref[dp ^ d] for d in range(4)]
    for h in range(KVH):
        examples = [part[h].astype(jnp.float32) for part in parts]
        for r in range(8):
            for j in range(2):
                total = jnp.zeros(examples[0].shape, jnp.float32)
                for d in range(4):
                    total += jnp.where(tasks[d] == first + r * 2 + j, examples[d], 0.0)
                out_ref[r, j, h] = total.astype(jnp.bfloat16)


def route(tasks, parts):
    return pl.pallas_call(
        route_kernel,
        out_shape=jax.ShapeDtypeStruct((8, 2, KVH, 32, HD), jnp.bfloat16),
        in_specs=[SMEM] + [VMEM] * 4,
        out_specs=VMEM,
        compiler_params=params(),
        name="route",
    )(tasks, *parts)


def banks_kernel(banks_ref, key_ref, value_ref):
    for r in range(8):
        out_ref = key_ref if r < 4 else value_ref
        rows = slice(r % 4 * 32, r % 4 * 32 + 32)
        for j in range(2):
            for h in range(KVH):
                out_ref[j, rows, h * HD : (h + 1) * HD] = banks_ref[r, j, h].astype(jnp.float32)


def banks_out(banks):
    shape = jax.ShapeDtypeStruct((2, PROMPT, KVH * HD), jnp.float32)
    return pl.pallas_call(
        banks_kernel,
        out_shape=(shape, shape),
        compiler_params=params(),
        name="banks_out",
    )(banks)


def heads_kernel(*refs):
    out_ref = refs[KVH]
    zh = lax.axis_index("zh")
    for d in range(KVH):
        h = (zh + d) % KVH
        out_ref[0, :, pl.ds(pl.multiple_of(h * WIDE, WIDE), WIDE)] = refs[d][...]


def heads_out(parts):
    return pl.pallas_call(
        heads_kernel,
        out_shape=jax.ShapeDtypeStruct((1, TOK, KVH * WIDE), jnp.bfloat16),
        compiler_params=params(),
        name="heads_out",
    )(*parts)


def swap(value, axis):
    return lax.ppermute(value, axis, [(0, 1), (1, 0)])


def from_left(value):
    return lax.ppermute(value, "x", [(i, (i + 1) % 4) for i in range(4)])


def from_right(value):
    return lax.ppermute(value, "x", [(i, (i - 1) % 4) for i in range(4)])


def crosswise(value, step):
    pairs = [(x * 2 + y, (x + step) % 4 * 2 + 1 - y) for x in range(4) for y in range(2)]
    return lax.ppermute(value, ("x", "y"), pairs)


def turned(parts, sign):
    moved = [parts[0]]
    for d in range(1, KVH):
        moved.append(
            lax.ppermute(parts[d], "zh", [(i, (i + sign * d) % 4) for i in range(4)])
        )
    return moved


def exchange(blocks, axes):
    return lax.all_to_all(blocks, axes, 0, 0, tiled=True)


def choose(index, own, others):
    chosen = own
    for position, other in others:
        chosen = jnp.where(index == position, other, chosen)
    return chosen


def step(queries, keys, values, segments, task_ids, prompt_keys, prompt_values, grad_out):
    dp, zh, zl, x, y = (lax.axis_index(name) for name in ALL)
    owner = task_ids[dp] // 2
    own_zh, own_zl, own_x, own_y = owner // 16, (owner // 8) % 2, (owner // 2) % 4, owner % 2

    payload = keys_payload(keys, values, segments)
    own = exchange(payload, ("zh", "zl"))
    q, go, prompts = rows_payload(
        task_ids, queries, grad_out, prompt_keys, prompt_values
    )
    prompts = turned(prompts, 1)

    beside = swap(own, "y")
    left = from_left(own)
    right = from_right(own)
    q = turned(q, 1)
    across = from_left(left)
    beside_across = crosswise(right, -1)
    beside_left = from_left(beside)
    beside_right = from_right(beside)
    go = turned(go, 1)

    prompt = choose((zh - own_zh) % KVH, prompts[0], list(enumerate(prompts))[1:])
    flip_zl, flip_y = (own_zl != zl).astype(jnp.int32), (own_y != y).astype(jnp.int32)
    both = lax.ppermute(prompt, ("zl", "y"), [(i, 3 - i) for i in range(4)])
    flipped = swap(prompt, "zl")
    beyond = swap(prompt, "y")
    prompt = choose(flip_zl * 2 + flip_y, prompt, [(2, flipped), (1, beyond), (3, both)])
    far = lax.ppermute(prompt, "x", [(i, (i + 2) % 4) for i in range(4)])
    sides = [((x + 3) % 4, from_left(prompt))]
    sides.append(((x + 1) % 4, from_right(prompt)))
    prompt = choose(own_x, prompt, sides + [((x + 2) % 4, far)])

    state = attend_first((0, 1, 2, 3), q, (own, beside, left, right))
    attended, grads = attend_last(
        (4, 5, 6, 7),
        q,
        go,
        state,
        own,
        prompt,
        (across, beside_left, beside_right, beside_across),
    )

    attended = turned(attended, -1)
    pieces = exchange(grads.reshape(8, 32, HD), ("x", "y"))
    sent = exchange(summed(pieces), ("zh", "zl"))
    mine = pairs_summed(sent)
    parts = [mine]
    for d in range(1, 4):
        parts.append(lax.ppermute(mine, "dp", [(i, i ^ d) for i in range(4)]))
    routed = route(task_ids, parts)
    banks = exchange(routed, ("x", "y"))
    key_grad, value_grad = banks_out(banks)
    return heads_out(attended), key_grad, value_grad


def solution(mesh):
    split = Mesh(mesh.devices.reshape(4, 4, 2, 4, 2), ALL)
    return jax.shard_map(
        step,
        mesh=split,
        in_specs=(
            P("dp", SEQ, None),
            P("dp", SEQ, None),
            P("dp", SEQ, None),
            P("dp", SEQ),
            P(),
            P(SEQ, None, None),
            P(SEQ, None, None),
            P("dp", SEQ, None),
        ),
        out_specs=(P("dp", SEQ, None), P(SEQ, None, None), P(SEQ, None, None)),
        check_vma=False,
    )
```

```python
import math

import jax
import jax.numpy as jnp
from jax import lax
from jax.experimental import pallas as pl
from jax.experimental.pallas import tpu as pltpu
from jax.sharding import Mesh
from jax.sharding import PartitionSpec as P

KVH = 4
GROUP = 4
HD = 128
PROMPT = 128
TOK = 128
WIDE = GROUP * HD
ZS = 8
CHUNK = 272
SEQ = ("zh", "zl", "x", "y")
ALL = ("dp", "zh", "zl", "x", "y")
SCALE = 1.0 / math.sqrt(HD)
LOG2E = math.log2(math.e)
FACTOR = SCALE * LOG2E
HIDDEN = -1e30
SPLIT = 2


ORDER = [(0, 0), (1, 0), (0, -1), (0, 1), (0, 2), (1, -1), (1, 1), (1, 2)]

VMEM = pl.BlockSpec(memory_space=pltpu.VMEM)
SMEM = pl.BlockSpec(memory_space=pltpu.SMEM)


HBM = pl.BlockSpec(memory_space=pltpu.HBM)


def params(mib=24):
    return pltpu.CompilerParams(vmem_limit_bytes=mib * 1024 * 1024)


def dot_nt(a, b):
    return lax.dot_general(a, b, (((1,), (1,)), ((), ())), preferred_element_type=jnp.float32)


def dot_tn(a, b):
    return lax.dot_general(a, b, (((0,), (0,)), ((), ())), preferred_element_type=jnp.float32)


def dot_nn(a, b):
    return lax.dot_general(a, b, (((1,), (0,)), ((), ())), preferred_element_type=jnp.float32)


def stacked_heads(block):
    return jnp.concatenate([block[:, g * HD : (g + 1) * HD] for g in range(GROUP)], axis=0)


def keys_kernel(keys_ref, values_ref, segments_ref, out_ref, seg_ref, sems):
    copies = [pltpu.make_async_copy(segments_ref, seg_ref, sems.at[0])]
    for z in range(ZS):
        cols = pl.ds(z // 2 * HD, HD)
        for n, source in enumerate((keys_ref, values_ref)):
            target = out_ref.at[z, pl.ds(n * TOK, TOK), :]
            copies.append(
                pltpu.make_async_copy(source.at[0, :, cols], target, sems.at[1 + 2 * z + n])
            )
    for copy in copies:
        copy.start()
    copies[0].wait()
    seg = seg_ref[...].astype(jnp.float32).astype(jnp.bfloat16)
    for z in range(ZS):
        out_ref[z, 2 * TOK : CHUNK, :] = jnp.broadcast_to(seg, (CHUNK - 2 * TOK, TOK))
    for copy in copies[1:]:
        copy.wait()


def keys_payload(keys, values, segments):
    return pl.pallas_call(
        keys_kernel,
        out_shape=jax.ShapeDtypeStruct((ZS, CHUNK, HD), jnp.bfloat16),
        in_specs=[HBM, HBM, HBM],
        out_specs=VMEM,
        scratch_shapes=[
            pltpu.VMEM((1, TOK), jnp.int32),
            pltpu.SemaphoreType.DMA((1 + 2 * ZS,)),
        ],
        compiler_params=params(),
        name="keys_payload",
    )(*in_hbm(keys, values, segments))


def rows_kernel(tasks_ref, queries_ref, go_ref, pk_ref, pv_ref, *rest):
    outs, sems = rest[: 3 * KVH], rest[3 * KVH]
    slot = tasks_ref[lax.axis_index("dp")] % 2
    zh = lax.axis_index("zh")
    half = PROMPT // 2
    copies = []

    def add(source, target):
        copies.append(pltpu.make_async_copy(source, target, sems.at[len(copies)]))

    for d in range(KVH):
        h = (zh + d) % KVH
        cols = pl.ds(pl.multiple_of(h * WIDE, WIDE), WIDE)
        q_out, go_out, prompt_out = outs[d], outs[KVH + d], outs[2 * KVH + d]
        add(queries_ref.at[0, :, cols], q_out)
        own = pl.ds(pl.multiple_of(h * HD, HD), HD)
        for n, bank in enumerate((pk_ref, pv_ref)):
            for s in range(2):
                place = pl.ds((2 * n + s) * HD, HD)
                add(
                    bank.at[slot, pl.ds(s * half, half), own],
                    prompt_out.at[:, place],
                )
        add(go_ref.at[0, :, cols], go_out)
    for copy in copies:
        copy.start()
    for copy in copies:
        copy.wait()


def rows_payload(tasks, queries, go, prompt_keys, prompt_values):
    outs = pl.pallas_call(
        rows_kernel,
        out_shape=[jax.ShapeDtypeStruct((TOK, WIDE), jnp.bfloat16)] * (2 * KVH)
        + [jax.ShapeDtypeStruct((PROMPT // 2, WIDE), jnp.bfloat16)] * KVH,
        in_specs=[SMEM, HBM, HBM, HBM, HBM],
        out_specs=[VMEM] * (3 * KVH),
        scratch_shapes=[pltpu.SemaphoreType.DMA((6 * KVH,))],
        compiler_params=params(),
        name="rows_payload",
    )(tasks, *in_hbm(queries, go, prompt_keys, prompt_values))
    return outs[:KVH], outs[KVH : 2 * KVH], outs[2 * KVH :]


class Bundle:
    def __init__(self, ref):
        self.ref = ref

    def keys(self, z):
        return self.ref[z, 0:TOK, :]

    def values(self, z):
        return self.ref[z, TOK : 2 * TOK, :]

    def segments(self, z):
        return self.ref[z, 2 * TOK : CHUNK, :].astype(jnp.float32)[0:1]


def accumulate(scores, wide, acc_ref, peak_ref, rows):
    old = peak_ref[rows]
    peak = jnp.maximum(old, jnp.max(scores, axis=1, keepdims=True))
    weights = jnp.exp2((scores - peak) * FACTOR).astype(jnp.bfloat16)
    shrink = jnp.exp2((old - peak) * FACTOR)
    acc_ref[rows] = acc_ref[rows] * shrink + dot_nn(weights, wide)
    peak_ref[rows] = peak


def absorb(bundles, j, q, seg_q, diagonal, acc_ref, peak_ref):
    zl, x, y = (lax.axis_index(name) for name in ("zl", "x", "y"))
    count = len(bundles) * 2 * TOK
    keys, values, visible = [], [], []
    for e in range(2):
        z = 2 * j + e
        for n, part in bundles.items():
            keys.append(part.keys(z))
            values.append(part.values(z))
            seg = part.segments(z)
            if diagonal and n != 0:
                b, c = ORDER[n]
                before = ((x + c + 4) % 4 * 2 + (y + b) % 2) < x * 2 + y
                shown = (zl > e) | ((zl == e) & before)
                seg = jnp.where(shown, seg, -1.0)
            same = seg_q == seg
            if diagonal and n == 0:
                reach = jnp.where(zl == e, 0, jnp.where(zl > e, TOK, -TOK))
                rows = lax.broadcasted_iota(jnp.int32, (TOK, TOK), 0)
                cols = lax.broadcasted_iota(jnp.int32, (TOK, TOK), 1)
                same = same & (cols - rows <= reach)
            visible.append(same)
    keys = jnp.concatenate(keys, axis=0)
    values = jnp.concatenate(values, axis=0)
    visible = jnp.concatenate(visible, axis=1)[None]
    wide = jnp.concatenate([values, jnp.ones(values.shape, jnp.bfloat16)], axis=1)
    size = GROUP * TOK // SPLIT
    scores = []
    for g in range(SPLIT):
        part = dot_nt(q[g * size : (g + 1) * size], keys).reshape(size // TOK, TOK, count)
        scores.append(jnp.where(visible, part, HIDDEN).reshape(size, count))
    for g in range(SPLIT):
        rows = slice(g * size, (g + 1) * size)
        accumulate(scores[g], wide, acc_ref, peak_ref, rows)


def sweep(bundles, own_ref, q, k, acc_ref, peak_ref):
    seg = own_ref[2 * k + lax.axis_index("zl"), 2 * TOK :, :].astype(jnp.float32)[0:1]
    seg_q = jnp.transpose(jnp.broadcast_to(seg, (TOK, TOK)))
    absorb(bundles, k, q, seg_q, True, acc_ref, peak_ref)

    def earlier(j, carry):
        absorb(bundles, j, q, seg_q, False, acc_ref, peak_ref)
        return carry

    lax.fori_loop(0, k, earlier, 0)


def first_kernel(names, *refs):
    q_refs, refs = refs[:KVH], refs[KVH:]
    bundles = {n: Bundle(ref) for n, ref in zip(names, refs)}
    refs = refs[len(names) :]
    out_ref, q_ref, state_ref, acc_ref, peak_ref, sems = refs
    own_ref = bundles[0].ref
    zh = lax.axis_index("zh")
    for d in range(KVH):
        q_ref[d] = stacked_heads(q_refs[d][...])

    def saved(d):
        return pltpu.make_async_copy(state_ref.at[d], out_ref.at[d], sems.at[d])

    def per_block(d, carry):
        acc_ref[...] = jnp.zeros_like(acc_ref)
        peak_ref[...] = jnp.full_like(peak_ref, HIDDEN)
        sweep(bundles, own_ref, q_ref[d], (zh - d + KVH) % KVH, acc_ref, peak_ref)
        state_ref[d, :, :HD] = acc_ref[:, :HD]
        lanes = lax.broadcasted_iota(jnp.int32, (GROUP * TOK, HD), 1)
        state_ref[d, :, HD:] = jnp.where(lanes < HD // 2, acc_ref[:, HD:], peak_ref[...])
        saved(d).start()
        return carry

    lax.fori_loop(0, KVH, per_block, 0)
    for d in range(KVH):
        saved(d).wait()


STATE = (KVH, GROUP * TOK, 2 * HD)


def cost(count):
    work = GROUP * TOK * HD * 4 * count * 2 * TOK * 10
    return pl.CostEstimate(flops=work, transcendentals=work // 512, bytes_accessed=1 << 22)


def attend_first(names, q, arrays):
    return pl.pallas_call(
        lambda *refs: first_kernel(names, *refs),
        out_shape=jax.ShapeDtypeStruct(STATE, jnp.float32),
        in_specs=[VMEM] * (KVH + len(arrays)),
        out_specs=pl.BlockSpec(memory_space=pltpu.HBM),
        scratch_shapes=[
            pltpu.VMEM((KVH, GROUP * TOK, HD), jnp.bfloat16),
            pltpu.VMEM(STATE, jnp.float32),
            pltpu.VMEM((GROUP * TOK, 2 * HD), jnp.float32),
            pltpu.VMEM((GROUP * TOK, 1), jnp.float32),
            pltpu.SemaphoreType.DMA((KVH,)),
        ],
        compiler_params=params(),
        cost_estimate=cost(len(names)),
        name="attend_first",
    )(*q, *arrays)


def last_kernel(names, *refs):
    q_refs, go_refs, refs = refs[:KVH], refs[KVH : 2 * KVH], refs[2 * KVH :]
    in_ref, own_ref, prompt_ref, *refs = refs
    bundles = {n: Bundle(ref) for n, ref in zip(names, refs)}
    refs = refs[len(names) :]
    att_refs, refs = refs[:KVH], refs[KVH:]
    grads_ref, q_ref, go_ref, state_ref, acc_ref, peak_ref, scores_ref, sems = refs
    zh = lax.axis_index("zh")

    def loaded(d):
        return pltpu.make_async_copy(in_ref.at[d], state_ref.at[d], sems.at[d])

    for d in range(KVH):
        loaded(d).start()
    for d in range(KVH):
        q_ref[d] = stacked_heads(q_refs[d][...])
        go_ref[d] = stacked_heads(go_refs[d][...])
    prompt_k = jnp.concatenate([prompt_ref[:, 0:HD], prompt_ref[:, HD : 2 * HD]], axis=0)
    prompt_v = jnp.concatenate([prompt_ref[:, 2 * HD : 3 * HD], prompt_ref[:, 3 * HD :]], axis=0)
    ones = jnp.ones(prompt_v.shape, jnp.bfloat16)
    prompt_wide = jnp.concatenate([prompt_v, ones], axis=1)

    blocks = range(KVH)
    for d in blocks:
        loaded(d).wait()
    for d in blocks:
        acc_ref[d, :, :HD] = state_ref[d, :, :HD]
        acc_ref[d, :, HD:] = jnp.broadcast_to(state_ref[d, :, HD : HD + 1], (GROUP * TOK, HD))
        peak_ref[d] = state_ref[d, :, 2 * HD - 1 :]
        scores_ref[d] = dot_nt(q_ref[d], prompt_k)
    for d in blocks:
        accumulate(scores_ref[d], prompt_wide, acc_ref.at[d], peak_ref.at[d], slice(None))

    def per_block(d, carry):
        k = (zh - d + KVH) % KVH
        sweep(bundles, own_ref, q_ref[d], k, acc_ref.at[d], peak_ref.at[d])
        return carry

    lax.fori_loop(0, KVH, per_block, 0)
    lows, probs_lows = [], []
    for d in blocks:
        norm = acc_ref[d, :, HD:]
        attended = (acc_ref[d, :, :HD] / norm).astype(jnp.bfloat16)
        for g in range(GROUP):
            att_refs[d][:, g * HD : (g + 1) * HD] = attended[g * TOK : (g + 1) * TOK]
        go = go_ref[d]
        delta = jnp.sum(
            go.astype(jnp.float32) * attended.astype(jnp.float32), axis=1, keepdims=True
        )
        log_norm = peak_ref[d] * FACTOR + jnp.log2(norm)
        probs = jnp.exp2(scores_ref[d] * FACTOR - log_norm)
        score_grad = probs * (dot_nt(go, prompt_v) - delta)
        lows.append(score_grad.astype(jnp.bfloat16))
        probs_lows.append(probs.astype(jnp.bfloat16))
    everything = (KVH * GROUP * TOK, HD)
    key_part = dot_tn(jnp.concatenate(lows, axis=0), q_ref[...].reshape(everything)) * SCALE
    value_part = dot_tn(jnp.concatenate(probs_lows, axis=0), go_ref[...].reshape(everything))
    grads_ref[0:PROMPT, :] = key_part.astype(jnp.bfloat16)
    grads_ref[PROMPT:, :] = value_part.astype(jnp.bfloat16)


def attend_last(names, q, go, state, own, prompt, arrays):
    outs = pl.pallas_call(
        lambda *refs: last_kernel(names, *refs),
        out_shape=[jax.ShapeDtypeStruct((TOK, WIDE), jnp.bfloat16)] * KVH
        + [jax.ShapeDtypeStruct((2 * PROMPT, HD), jnp.bfloat16)],
        in_specs=[VMEM] * (2 * KVH)
        + [pl.BlockSpec(memory_space=pltpu.HBM)]
        + [VMEM] * (2 + len(arrays)),
        out_specs=[VMEM] * (KVH + 1),
        scratch_shapes=[
            pltpu.VMEM((KVH, GROUP * TOK, HD), jnp.bfloat16),
            pltpu.VMEM((KVH, GROUP * TOK, HD), jnp.bfloat16),
            pltpu.VMEM(STATE, jnp.float32),
            pltpu.VMEM((KVH, GROUP * TOK, 2 * HD), jnp.float32),
            pltpu.VMEM((KVH, GROUP * TOK, 1), jnp.float32),
            pltpu.VMEM((KVH, GROUP * TOK, HD), jnp.float32),
            pltpu.SemaphoreType.DMA((KVH,)),
        ],
        compiler_params=params(),
        cost_estimate=cost(len(names) + 1),
        name="attend_last",
    )(*q, *go, state, own, prompt, *arrays)
    return outs[:KVH], outs[KVH]


def sum_kernel(pieces_ref, out_ref):
    total = pieces_ref[0].astype(jnp.float32)
    for r in range(1, 8):
        total += pieces_ref[r].astype(jnp.float32)
    for r in range(8):
        out_ref[r] = total.astype(jnp.bfloat16)


def summed(pieces):
    return pl.pallas_call(
        sum_kernel,
        out_shape=jax.ShapeDtypeStruct((8, 32, HD), jnp.bfloat16),
        in_specs=[VMEM],
        out_specs=VMEM,
        compiler_params=params(),
        name="summed",
    )(pieces)


def pairs_kernel(sent_ref, out_ref):
    for h in range(KVH):
        total = sent_ref[2 * h].astype(jnp.float32) + sent_ref[2 * h + 1].astype(jnp.float32)
        out_ref[h] = total.astype(jnp.bfloat16)


def pairs_summed(sent):
    return pl.pallas_call(
        pairs_kernel,
        out_shape=jax.ShapeDtypeStruct((KVH, 32, HD), jnp.bfloat16),
        in_specs=[VMEM],
        out_specs=VMEM,
        compiler_params=params(),
        name="pairs_summed",
    )(sent)


def route_kernel(tasks_ref, *refs):
    parts, out_ref = refs[:4], refs[4]
    dp = lax.axis_index("dp")
    first = (lax.axis_index("zh") * 2 + lax.axis_index("zl")) * 16
    tasks = [tasks_ref[dp ^ d] for d in range(4)]
    for h in range(KVH):
        examples = [part[h].astype(jnp.float32) for part in parts]
        for r in range(8):
            for j in range(2):
                total = jnp.zeros(examples[0].shape, jnp.float32)
                for d in range(4):
                    total += jnp.where(tasks[d] == first + r * 2 + j, examples[d], 0.0)
                out_ref[r, j, h] = total.astype(jnp.bfloat16)


def route(tasks, parts):
    return pl.pallas_call(
        route_kernel,
        out_shape=jax.ShapeDtypeStruct((8, 2, KVH, 32, HD), jnp.bfloat16),
        in_specs=[SMEM] + [VMEM] * 4,
        out_specs=VMEM,
        compiler_params=params(),
        name="route",
    )(tasks, *parts)


def banks_kernel(banks_ref, key_ref, value_ref):
    for r in range(8):
        out_ref = key_ref if r < 4 else value_ref
        rows = slice(r % 4 * 32, r % 4 * 32 + 32)
        for j in range(2):
            for h in range(KVH):
                out_ref[j, rows, h * HD : (h + 1) * HD] = banks_ref[r, j, h].astype(jnp.float32)


def banks_out(banks):
    shape = jax.ShapeDtypeStruct((2, PROMPT, KVH * HD), jnp.float32)
    return pl.pallas_call(
        banks_kernel,
        out_shape=(shape, shape),
        compiler_params=params(),
        name="banks_out",
    )(banks)


def heads_kernel(*refs):
    out_ref = refs[KVH]
    zh = lax.axis_index("zh")
    for d in range(KVH):
        h = (zh + d) % KVH
        out_ref[0, :, pl.ds(pl.multiple_of(h * WIDE, WIDE), WIDE)] = refs[d][...]


def heads_out(parts):
    return pl.pallas_call(
        heads_kernel,
        out_shape=jax.ShapeDtypeStruct((1, TOK, KVH * WIDE), jnp.bfloat16),
        compiler_params=params(),
        name="heads_out",
    )(*parts)


def swap(value, axis):
    return lax.ppermute(value, axis, [(0, 1), (1, 0)])


def from_left(value):
    return lax.ppermute(value, "x", [(i, (i + 1) % 4) for i in range(4)])


def from_right(value):
    return lax.ppermute(value, "x", [(i, (i - 1) % 4) for i in range(4)])


def crosswise(value, step):
    pairs = [(x * 2 + y, (x + step) % 4 * 2 + 1 - y) for x in range(4) for y in range(2)]
    return lax.ppermute(value, ("x", "y"), pairs)


def turned(parts, sign):
    moved = [parts[0]]
    for d in range(1, KVH):
        moved.append(
            lax.ppermute(parts[d], "zh", [(i, (i + sign * d) % 4) for i in range(4)])
        )
    return moved


def exchange(blocks, axes):
    return lax.all_to_all(blocks, axes, 0, 0, tiled=True)


def choose_kernel(stage, tasks_ref, *refs):
    parts, out_ref = refs[:KVH], refs[KVH]
    owner = tasks_ref[lax.axis_index("dp")] // 2
    if stage == "zh":
        wanted = (lax.axis_index("zh") + KVH - owner // 16) % KVH
    elif stage == "zl_y":
        zl, y = lax.axis_index("zl"), lax.axis_index("y")
        wanted = ((owner // 8 + zl) % 2) * 2 + (owner + y) % 2
    else:
        wanted = (lax.axis_index("x") + 4 - (owner // 2) % 4) % 4
    for n in range(KVH):

        @pl.when(wanted == n)
        def _():
            out_ref[...] = parts[n][...]


def choose(stage, tasks, parts):
    return pl.pallas_call(
        lambda *refs: choose_kernel(stage, *refs),
        out_shape=jax.ShapeDtypeStruct(parts[0].shape, parts[0].dtype),
        in_specs=[SMEM] + [VMEM] * KVH,
        out_specs=VMEM,
        compiler_params=params(4),
    )(tasks, *parts)


def in_hbm(*arrays):
    return [pltpu.with_memory_space_constraint(array, pltpu.HBM) for array in arrays]


def step(queries, keys, values, segments, task_ids, prompt_keys, prompt_values, grad_out):
    payload = keys_payload(keys, values, segments)
    own = exchange(payload, ("zh", "zl"))
    q, go, prompts = rows_payload(
        task_ids, queries, grad_out, prompt_keys, prompt_values
    )
    prompts = turned(prompts, 1)

    beside = swap(own, "y")
    left = from_left(own)
    right = from_right(own)
    q = turned(q, 1)
    across = from_left(left)
    beside_across = crosswise(right, -1)
    beside_left = from_left(beside)
    beside_right = from_right(beside)
    go = turned(go, 1)

    prompt = choose("zh", task_ids, prompts)
    both = lax.ppermute(prompt, ("zl", "y"), [(i, 3 - i) for i in range(4)])
    flipped = swap(prompt, "zl")
    beyond = swap(prompt, "y")
    prompt = choose("zl_y", task_ids, (prompt, beyond, flipped, both))
    far = lax.ppermute(prompt, "x", [(i, (i + 2) % 4) for i in range(4)])
    prompt_left = from_left(prompt)
    prompt_right = from_right(prompt)
    prompt = choose("x", task_ids, (prompt, prompt_left, far, prompt_right))

    state = attend_first((0, 1, 2, 3), q, (own, beside, left, right))
    attended, grads = attend_last(
        (4, 5, 6, 7),
        q,
        go,
        state,
        own,
        prompt,
        (across, beside_left, beside_right, beside_across),
    )

    attended = turned(attended, -1)
    pieces = exchange(grads.reshape(8, 32, HD), ("x", "y"))
    sent = exchange(summed(pieces), ("zh", "zl"))
    mine = pairs_summed(sent)
    parts = [mine]
    for d in range(1, 4):
        parts.append(lax.ppermute(mine, "dp", [(i, i ^ d) for i in range(4)]))
    routed = route(task_ids, parts)
    banks = exchange(routed, ("x", "y"))
    key_grad, value_grad = banks_out(banks)
    return heads_out(attended), key_grad, value_grad


def solution(mesh):
    split = Mesh(mesh.devices.reshape(4, 4, 2, 4, 2), ALL)
    return jax.shard_map(
        step,
        mesh=split,
        in_specs=(
            P("dp", SEQ, None),
            P("dp", SEQ, None),
            P("dp", SEQ, None),
            P("dp", SEQ),
            P(),
            P(SEQ, None, None),
            P(SEQ, None, None),
            P("dp", SEQ, None),
        ),
        out_specs=(P("dp", SEQ, None), P(SEQ, None, None), P(SEQ, None, None)),
        check_vma=False,
    )
```

```python
import math

import jax
import jax.numpy as jnp
from jax import lax
from jax.experimental import pallas as pl
from jax.experimental.pallas import tpu as pltpu
from jax.sharding import Mesh
from jax.sharding import PartitionSpec as P

KVH = 4
GROUP = 4
HD = 128
PROMPT = 128
TOK = 128
WIDE = GROUP * HD
ZS = 8
CHUNK = 272
SEQ = ("zh", "zl", "x", "y")
ALL = ("dp", "zh", "zl", "x", "y")
SCALE = 1.0 / math.sqrt(HD)
LOG2E = math.log2(math.e)
FACTOR = SCALE * LOG2E
HIDDEN = -1e30
SPLIT = 2


ORDER = [(0, 0), (1, 0), (0, -1), (0, 1), (0, 2), (1, -1), (1, 1), (1, 2)]

VMEM = pl.BlockSpec(memory_space=pltpu.VMEM)
SMEM = pl.BlockSpec(memory_space=pltpu.SMEM)


HBM = pl.BlockSpec(memory_space=pltpu.HBM)


def params(mib=24):
    return pltpu.CompilerParams(vmem_limit_bytes=mib * 1024 * 1024)


def dot_nt(a, b):
    return lax.dot_general(a, b, (((1,), (1,)), ((), ())), preferred_element_type=jnp.float32)


def dot_tn(a, b):
    return lax.dot_general(a, b, (((0,), (0,)), ((), ())), preferred_element_type=jnp.float32)


def dot_nn(a, b):
    return lax.dot_general(a, b, (((1,), (0,)), ((), ())), preferred_element_type=jnp.float32)


def stacked_heads(block):
    return jnp.concatenate([block[:, g * HD : (g + 1) * HD] for g in range(GROUP)], axis=0)


def keys_kernel(keys_ref, values_ref, segments_ref, out_ref, seg_ref, sems):
    copies = [pltpu.make_async_copy(segments_ref, seg_ref, sems.at[0])]
    for z in range(ZS):
        cols = pl.ds(z // 2 * HD, HD)
        for n, source in enumerate((keys_ref, values_ref)):
            target = out_ref.at[z, pl.ds(n * TOK, TOK), :]
            copies.append(
                pltpu.make_async_copy(source.at[0, :, cols], target, sems.at[1 + 2 * z + n])
            )
    for copy in copies:
        copy.start()
    copies[0].wait()
    seg = seg_ref[...].astype(jnp.float32).astype(jnp.bfloat16)
    for z in range(ZS):
        out_ref[z, 2 * TOK : CHUNK, :] = jnp.broadcast_to(seg, (CHUNK - 2 * TOK, TOK))
    for copy in copies[1:]:
        copy.wait()


def keys_payload(keys, values, segments):
    return pl.pallas_call(
        keys_kernel,
        out_shape=jax.ShapeDtypeStruct((ZS, CHUNK, HD), jnp.bfloat16),
        in_specs=[HBM, HBM, HBM],
        out_specs=VMEM,
        scratch_shapes=[
            pltpu.VMEM((1, TOK), jnp.int32),
            pltpu.SemaphoreType.DMA((1 + 2 * ZS,)),
        ],
        compiler_params=params(),
        name="keys_payload",
    )(*in_hbm(keys, values, segments))


def rows_kernel(tasks_ref, queries_ref, go_ref, pk_ref, pv_ref, *rest):
    outs, sems = rest[: 3 * KVH], rest[3 * KVH]
    slot = tasks_ref[lax.axis_index("dp")] % 2
    zh = lax.axis_index("zh")
    half = PROMPT // 2
    copies = []

    def add(source, target):
        copies.append(pltpu.make_async_copy(source, target, sems.at[len(copies)]))

    for d in range(KVH):
        h = (zh + d) % KVH
        cols = pl.ds(pl.multiple_of(h * WIDE, WIDE), WIDE)
        q_out, go_out, prompt_out = outs[d], outs[KVH + d], outs[2 * KVH + d]
        add(queries_ref.at[0, :, cols], q_out)
        own = pl.ds(pl.multiple_of(h * HD, HD), HD)
        for n, bank in enumerate((pk_ref, pv_ref)):
            for s in range(2):
                place = pl.ds((2 * n + s) * HD, HD)
                add(
                    bank.at[slot, pl.ds(s * half, half), own],
                    prompt_out.at[:, place],
                )
        add(go_ref.at[0, :, cols], go_out)
    for copy in copies:
        copy.start()
    for copy in copies:
        copy.wait()


def rows_payload(tasks, queries, go, prompt_keys, prompt_values):
    outs = pl.pallas_call(
        rows_kernel,
        out_shape=[jax.ShapeDtypeStruct((TOK, WIDE), jnp.bfloat16)] * (2 * KVH)
        + [jax.ShapeDtypeStruct((PROMPT // 2, WIDE), jnp.bfloat16)] * KVH,
        in_specs=[SMEM, HBM, HBM, HBM, HBM],
        out_specs=[VMEM] * (3 * KVH),
        scratch_shapes=[pltpu.SemaphoreType.DMA((6 * KVH,))],
        compiler_params=params(),
        name="rows_payload",
    )(tasks, *in_hbm(queries, go, prompt_keys, prompt_values))
    return outs[:KVH], outs[KVH : 2 * KVH], outs[2 * KVH :]


class Bundle:
    def __init__(self, ref):
        self.ref = ref

    def keys(self, z):
        return self.ref[z, 0:TOK, :]

    def values(self, z):
        return self.ref[z, TOK : 2 * TOK, :]

    def segments(self, z):
        return self.ref[z, 2 * TOK : CHUNK, :].astype(jnp.float32)[0:1]


def accumulate(scores, wide, acc_ref, peak_ref, rows):
    old = peak_ref[rows]
    peak = jnp.maximum(old, jnp.max(scores, axis=1, keepdims=True))
    weights = jnp.exp2((scores - peak) * FACTOR).astype(jnp.bfloat16)
    shrink = jnp.exp2((old - peak) * FACTOR)
    acc_ref[rows] = acc_ref[rows] * shrink + dot_nn(weights, wide)
    peak_ref[rows] = peak


def absorb(bundles, j, q, seg_q, diagonal, acc_ref, peak_ref):
    zl, x, y = (lax.axis_index(name) for name in ("zl", "x", "y"))
    count = len(bundles) * 2 * TOK
    keys, values, visible = [], [], []
    for e in range(2):
        z = 2 * j + e
        for n, part in bundles.items():
            keys.append(part.keys(z))
            values.append(part.values(z))
            seg = part.segments(z)
            if diagonal and n != 0:
                b, c = ORDER[n]
                before = ((x + c + 4) % 4 * 2 + (y + b) % 2) < x * 2 + y
                shown = (zl > e) | ((zl == e) & before)
                seg = jnp.where(shown, seg, -1.0)
            same = seg_q == seg
            if diagonal and n == 0:
                reach = jnp.where(zl == e, 0, jnp.where(zl > e, TOK, -TOK))
                rows = lax.broadcasted_iota(jnp.int32, (TOK, TOK), 0)
                cols = lax.broadcasted_iota(jnp.int32, (TOK, TOK), 1)
                same = same & (cols - rows <= reach)
            visible.append(same)
    keys = jnp.concatenate(keys, axis=0)
    values = jnp.concatenate(values, axis=0)
    visible = jnp.concatenate(visible, axis=1)[None]
    wide = jnp.concatenate([values, jnp.ones(values.shape, jnp.bfloat16)], axis=1)
    size = GROUP * TOK // SPLIT
    scores = []
    for g in range(SPLIT):
        part = dot_nt(q[g * size : (g + 1) * size], keys).reshape(size // TOK, TOK, count)
        scores.append(jnp.where(visible, part, HIDDEN).reshape(size, count))
    for g in range(SPLIT):
        rows = slice(g * size, (g + 1) * size)
        accumulate(scores[g], wide, acc_ref, peak_ref, rows)


def sweep(bundles, own_ref, q, k, acc_ref, peak_ref):
    seg = own_ref[2 * k + lax.axis_index("zl"), 2 * TOK :, :].astype(jnp.float32)[0:1]
    seg_q = jnp.transpose(jnp.broadcast_to(seg, (TOK, TOK)))
    absorb(bundles, k, q, seg_q, True, acc_ref, peak_ref)

    def earlier(j, carry):
        absorb(bundles, j, q, seg_q, False, acc_ref, peak_ref)
        return carry

    lax.fori_loop(0, k, earlier, 0)


def first_kernel(names, *refs):
    q_refs, refs = refs[:KVH], refs[KVH:]
    bundles = {n: Bundle(ref) for n, ref in zip(names, refs)}
    refs = refs[len(names) :]
    out_ref, q_ref, state_ref, acc_ref, peak_ref, sems = refs
    own_ref = bundles[0].ref
    zh = lax.axis_index("zh")
    for d in range(KVH):
        q_ref[d] = stacked_heads(q_refs[d][...])

    def saved(d):
        return pltpu.make_async_copy(state_ref.at[d], out_ref.at[d], sems.at[d])

    def per_block(d, carry):
        acc_ref[...] = jnp.zeros_like(acc_ref)
        peak_ref[...] = jnp.full_like(peak_ref, HIDDEN)
        sweep(bundles, own_ref, q_ref[d], (zh - d + KVH) % KVH, acc_ref, peak_ref)
        state_ref[d, :, :HD] = acc_ref[:, :HD]
        lanes = lax.broadcasted_iota(jnp.int32, (GROUP * TOK, HD), 1)
        state_ref[d, :, HD:] = jnp.where(lanes < HD // 2, acc_ref[:, HD:], peak_ref[...])
        saved(d).start()
        return carry

    lax.fori_loop(0, KVH, per_block, 0)
    for d in range(KVH):
        saved(d).wait()


STATE = (KVH, GROUP * TOK, 2 * HD)


def cost(count):
    work = GROUP * TOK * HD * 4 * count * 2 * TOK * 10
    return pl.CostEstimate(flops=work, transcendentals=work // 512, bytes_accessed=1 << 22)


def attend_first(names, q, arrays):
    return pl.pallas_call(
        lambda *refs: first_kernel(names, *refs),
        out_shape=jax.ShapeDtypeStruct(STATE, jnp.float32),
        in_specs=[VMEM] * (KVH + len(arrays)),
        out_specs=pl.BlockSpec(memory_space=pltpu.HBM),
        scratch_shapes=[
            pltpu.VMEM((KVH, GROUP * TOK, HD), jnp.bfloat16),
            pltpu.VMEM(STATE, jnp.float32),
            pltpu.VMEM((GROUP * TOK, 2 * HD), jnp.float32),
            pltpu.VMEM((GROUP * TOK, 1), jnp.float32),
            pltpu.SemaphoreType.DMA((KVH,)),
        ],
        compiler_params=params(),
        cost_estimate=cost(len(names)),
        name="attend_first",
    )(*q, *arrays)


def last_kernel(names, *refs):
    q_refs, go_refs, refs = refs[:KVH], refs[KVH : 2 * KVH], refs[2 * KVH :]
    in_ref, own_ref, prompt_ref, *refs = refs
    bundles = {n: Bundle(ref) for n, ref in zip(names, refs)}
    refs = refs[len(names) :]
    att_refs, refs = refs[:KVH], refs[KVH:]
    grads_ref, q_ref, go_ref, state_ref, acc_ref, peak_ref, scores_ref, sems = refs
    zh = lax.axis_index("zh")

    def loaded(d):
        return pltpu.make_async_copy(in_ref.at[d], state_ref.at[d], sems.at[d])

    for d in range(KVH):
        loaded(d).start()
    for d in range(KVH):
        q_ref[d] = stacked_heads(q_refs[d][...])
        go_ref[d] = stacked_heads(go_refs[d][...])
    prompt_k = jnp.concatenate([prompt_ref[:, 0:HD], prompt_ref[:, HD : 2 * HD]], axis=0)
    prompt_v = jnp.concatenate([prompt_ref[:, 2 * HD : 3 * HD], prompt_ref[:, 3 * HD :]], axis=0)
    ones = jnp.ones(prompt_v.shape, jnp.bfloat16)
    prompt_wide = jnp.concatenate([prompt_v, ones], axis=1)

    blocks = range(KVH)
    for d in blocks:
        loaded(d).wait()
    for d in blocks:
        acc_ref[d, :, :HD] = state_ref[d, :, :HD]
        acc_ref[d, :, HD:] = jnp.broadcast_to(state_ref[d, :, HD : HD + 1], (GROUP * TOK, HD))
        peak_ref[d] = state_ref[d, :, 2 * HD - 1 :]
        scores_ref[d] = dot_nt(q_ref[d], prompt_k)
    for d in blocks:
        accumulate(scores_ref[d], prompt_wide, acc_ref.at[d], peak_ref.at[d], slice(None))

    def per_block(d, carry):
        k = (zh - d + KVH) % KVH
        sweep(bundles, own_ref, q_ref[d], k, acc_ref.at[d], peak_ref.at[d])
        return carry

    lax.fori_loop(0, KVH, per_block, 0)
    lows, probs_lows = [], []
    for d in blocks:
        norm = acc_ref[d, :, HD:]
        attended = (acc_ref[d, :, :HD] / norm).astype(jnp.bfloat16)
        for g in range(GROUP):
            att_refs[d][:, g * HD : (g + 1) * HD] = attended[g * TOK : (g + 1) * TOK]
        go = go_ref[d]
        delta = jnp.sum(
            go.astype(jnp.float32) * attended.astype(jnp.float32), axis=1, keepdims=True
        )
        log_norm = peak_ref[d] * FACTOR + jnp.log2(norm)
        probs = jnp.exp2(scores_ref[d] * FACTOR - log_norm)
        score_grad = probs * (dot_nt(go, prompt_v) - delta)
        lows.append(score_grad.astype(jnp.bfloat16))
        probs_lows.append(probs.astype(jnp.bfloat16))
    everything = (KVH * GROUP * TOK, HD)
    key_part = dot_tn(jnp.concatenate(lows, axis=0), q_ref[...].reshape(everything)) * SCALE
    value_part = dot_tn(jnp.concatenate(probs_lows, axis=0), go_ref[...].reshape(everything))
    grads_ref[0:PROMPT, :] = key_part.astype(jnp.bfloat16)
    grads_ref[PROMPT:, :] = value_part.astype(jnp.bfloat16)


def attend_last(names, q, go, state, own, prompt, arrays):
    outs = pl.pallas_call(
        lambda *refs: last_kernel(names, *refs),
        out_shape=[jax.ShapeDtypeStruct((TOK, WIDE), jnp.bfloat16)] * KVH
        + [jax.ShapeDtypeStruct((2 * PROMPT, HD), jnp.bfloat16)],
        in_specs=[VMEM] * (2 * KVH)
        + [pl.BlockSpec(memory_space=pltpu.HBM)]
        + [VMEM] * (2 + len(arrays)),
        out_specs=[VMEM] * (KVH + 1),
        scratch_shapes=[
            pltpu.VMEM((KVH, GROUP * TOK, HD), jnp.bfloat16),
            pltpu.VMEM((KVH, GROUP * TOK, HD), jnp.bfloat16),
            pltpu.VMEM(STATE, jnp.float32),
            pltpu.VMEM((KVH, GROUP * TOK, 2 * HD), jnp.float32),
            pltpu.VMEM((KVH, GROUP * TOK, 1), jnp.float32),
            pltpu.VMEM((KVH, GROUP * TOK, HD), jnp.float32),
            pltpu.SemaphoreType.DMA((KVH,)),
        ],
        compiler_params=params(),
        cost_estimate=cost(len(names) + 1),
        name="attend_last",
    )(*q, *go, state, own, prompt, *arrays)
    return outs[:KVH], outs[KVH]


def sum_kernel(pieces_ref, out_ref):
    total = pieces_ref[0].astype(jnp.float32)
    for r in range(1, 8):
        total += pieces_ref[r].astype(jnp.float32)
    for r in range(8):
        out_ref[r] = total.astype(jnp.bfloat16)


def summed(pieces):
    return pl.pallas_call(
        sum_kernel,
        out_shape=jax.ShapeDtypeStruct((8, 32, HD), jnp.bfloat16),
        in_specs=[VMEM],
        out_specs=VMEM,
        compiler_params=params(),
        name="summed",
    )(pieces)


def pairs_kernel(sent_ref, out_ref):
    for h in range(KVH):
        total = sent_ref[2 * h].astype(jnp.float32) + sent_ref[2 * h + 1].astype(jnp.float32)
        out_ref[h] = total.astype(jnp.bfloat16)


def pairs_summed(sent):
    return pl.pallas_call(
        pairs_kernel,
        out_shape=jax.ShapeDtypeStruct((KVH, 32, HD), jnp.bfloat16),
        in_specs=[VMEM],
        out_specs=VMEM,
        compiler_params=params(),
        name="pairs_summed",
    )(sent)


def route_kernel(tasks_ref, *refs):
    parts, out_ref = refs[:4], refs[4]
    dp = lax.axis_index("dp")
    first = (lax.axis_index("zh") * 2 + lax.axis_index("zl")) * 16
    places = [tasks_ref[dp ^ d] - first for d in range(4)]
    here = [(place >= 0) & (place < 16) for place in places]
    out_ref[...] = jnp.zeros_like(out_ref)
    for d in range(4):

        @pl.when(here[d])
        def _():
            total = parts[d][...].astype(jnp.float32)
            for e in range(d):
                same = here[e] & (places[e] == places[d])
                total += jnp.where(same, parts[e][...].astype(jnp.float32), 0.0)
            out_ref[jnp.clip(places[d], 0, 15)] = total.astype(jnp.bfloat16)


def route(tasks, parts):
    return pl.pallas_call(
        route_kernel,
        out_shape=jax.ShapeDtypeStruct((16, KVH, 32, HD), jnp.bfloat16),
        in_specs=[SMEM] + [VMEM] * 4,
        out_specs=VMEM,
        compiler_params=params(),
        name="route",
    )(tasks, *parts)


def banks_kernel(banks_ref, key_ref, value_ref):
    for r in range(8):
        out_ref = key_ref if r < 4 else value_ref
        rows = slice(r % 4 * 32, r % 4 * 32 + 32)
        for j in range(2):
            for h in range(KVH):
                part = banks_ref[2 * r + j, h].astype(jnp.float32)
                out_ref[j, rows, h * HD : (h + 1) * HD] = part


def banks_out(banks):
    shape = jax.ShapeDtypeStruct((2, PROMPT, KVH * HD), jnp.float32)
    return pl.pallas_call(
        banks_kernel,
        out_shape=(shape, shape),
        compiler_params=params(),
        name="banks_out",
    )(banks)


def heads_kernel(*refs):
    out_ref = refs[KVH]
    zh = lax.axis_index("zh")
    for d in range(KVH):
        h = (zh + d) % KVH
        out_ref[0, :, pl.ds(pl.multiple_of(h * WIDE, WIDE), WIDE)] = refs[d][...]


def heads_out(parts):
    return pl.pallas_call(
        heads_kernel,
        out_shape=jax.ShapeDtypeStruct((1, TOK, KVH * WIDE), jnp.bfloat16),
        compiler_params=params(),
        name="heads_out",
    )(*parts)


def swap(value, axis):
    return lax.ppermute(value, axis, [(0, 1), (1, 0)])


def from_left(value):
    return lax.ppermute(value, "x", [(i, (i + 1) % 4) for i in range(4)])


def from_right(value):
    return lax.ppermute(value, "x", [(i, (i - 1) % 4) for i in range(4)])


def crosswise(value, step):
    pairs = [(x * 2 + y, (x + step) % 4 * 2 + 1 - y) for x in range(4) for y in range(2)]
    return lax.ppermute(value, ("x", "y"), pairs)


def turned(parts, sign):
    moved = [parts[0]]
    for d in range(1, KVH):
        moved.append(
            lax.ppermute(parts[d], "zh", [(i, (i + sign * d) % 4) for i in range(4)])
        )
    return moved


def exchange(blocks, axes):
    return lax.all_to_all(blocks, axes, 0, 0, tiled=True)


def choose_kernel(stage, tasks_ref, *refs):
    parts, out_ref = refs[:KVH], refs[KVH]
    owner = tasks_ref[lax.axis_index("dp")] // 2
    if stage == "zh":
        wanted = (lax.axis_index("zh") + KVH - owner // 16) % KVH
    elif stage == "zl_y":
        zl, y = lax.axis_index("zl"), lax.axis_index("y")
        wanted = ((owner // 8 + zl) % 2) * 2 + (owner + y) % 2
    else:
        wanted = (lax.axis_index("x") + 4 - (owner // 2) % 4) % 4
    for n in range(KVH):

        @pl.when(wanted == n)
        def _():
            out_ref[...] = parts[n][...]


def choose(stage, tasks, parts):
    return pl.pallas_call(
        lambda *refs: choose_kernel(stage, *refs),
        out_shape=jax.ShapeDtypeStruct(parts[0].shape, parts[0].dtype),
        in_specs=[SMEM] + [VMEM] * KVH,
        out_specs=VMEM,
        compiler_params=params(4),
    )(tasks, *parts)


def in_hbm(*arrays):
    return [pltpu.with_memory_space_constraint(array, pltpu.HBM) for array in arrays]


def step(queries, keys, values, segments, task_ids, prompt_keys, prompt_values, grad_out):
    payload = keys_payload(keys, values, segments)
    own = exchange(payload, ("zh", "zl"))
    q, go, prompts = rows_payload(
        task_ids, queries, grad_out, prompt_keys, prompt_values
    )
    prompts = turned(prompts, 1)

    beside = swap(own, "y")
    left = from_left(own)
    right = from_right(own)
    q = turned(q, 1)
    across = from_left(left)
    beside_across = crosswise(right, -1)
    beside_left = from_left(beside)
    beside_right = from_right(beside)
    go = turned(go, 1)

    prompt = choose("zh", task_ids, prompts)
    both = lax.ppermute(prompt, ("zl", "y"), [(i, 3 - i) for i in range(4)])
    flipped = swap(prompt, "zl")
    beyond = swap(prompt, "y")
    prompt = choose("zl_y", task_ids, (prompt, beyond, flipped, both))
    far = lax.ppermute(prompt, "x", [(i, (i + 2) % 4) for i in range(4)])
    prompt_left = from_left(prompt)
    prompt_right = from_right(prompt)
    prompt = choose("x", task_ids, (prompt, prompt_left, far, prompt_right))

    state = attend_first((0, 1, 2, 3), q, (own, beside, left, right))
    attended, grads = attend_last(
        (4, 5, 6, 7),
        q,
        go,
        state,
        own,
        prompt,
        (across, beside_left, beside_right, beside_across),
    )

    attended = turned(attended, -1)
    pieces = exchange(grads.reshape(8, 32, HD), ("x", "y"))
    sent = exchange(summed(pieces), ("zh", "zl"))
    mine = pairs_summed(sent)
    parts = [mine]
    for d in range(1, 4):
        parts.append(lax.ppermute(mine, "dp", [(i, i ^ d) for i in range(4)]))
    routed = route(task_ids, parts)
    banks = exchange(routed, ("x", "y"))
    key_grad, value_grad = banks_out(banks)
    return heads_out(attended), key_grad, value_grad


def solution(mesh):
    split = Mesh(mesh.devices.reshape(4, 4, 2, 4, 2), ALL)
    return jax.shard_map(
        step,
        mesh=split,
        in_specs=(
            P("dp", SEQ, None),
            P("dp", SEQ, None),
            P("dp", SEQ, None),
            P("dp", SEQ),
            P(),
            P(SEQ, None, None),
            P(SEQ, None, None),
            P("dp", SEQ, None),
        ),
        out_specs=(P("dp", SEQ, None), P(SEQ, None, None), P(SEQ, None, None)),
        check_vma=False,
    )
```

```python
import math

import jax
import jax.numpy as jnp
from jax import lax
from jax.experimental import pallas as pl
from jax.experimental.pallas import tpu as pltpu
from jax.sharding import Mesh
from jax.sharding import PartitionSpec as P

KVH = 4
GROUP = 4
HD = 128
PROMPT = 128
TOK = 128
WIDE = GROUP * HD
ZS = 8
CHUNK = 272
SEQ = ("zh", "zl", "x", "y")
ALL = ("dp", "zh", "zl", "x", "y")
SCALE = 1.0 / math.sqrt(HD)
LOG2E = math.log2(math.e)
FACTOR = SCALE * LOG2E
HIDDEN = -1e30
SPLIT = 2


ORDER = [(0, 0), (1, 0), (0, -1), (0, 1), (0, 2), (1, -1), (1, 1), (1, 2)]

VMEM = pl.BlockSpec(memory_space=pltpu.VMEM)
SMEM = pl.BlockSpec(memory_space=pltpu.SMEM)


HBM = pl.BlockSpec(memory_space=pltpu.HBM)


def params(mib=24):
    return pltpu.CompilerParams(vmem_limit_bytes=mib * 1024 * 1024)


def dot_nt(a, b):
    return lax.dot_general(a, b, (((1,), (1,)), ((), ())), preferred_element_type=jnp.float32)


def dot_tn(a, b):
    return lax.dot_general(a, b, (((0,), (0,)), ((), ())), preferred_element_type=jnp.float32)


def dot_nn(a, b):
    return lax.dot_general(a, b, (((1,), (0,)), ((), ())), preferred_element_type=jnp.float32)


def stacked_heads(block):
    return jnp.concatenate([block[:, g * HD : (g + 1) * HD] for g in range(GROUP)], axis=0)


def keys_kernel(keys_ref, values_ref, segments_ref, out_ref, seg_ref, sems):
    copies = [pltpu.make_async_copy(segments_ref, seg_ref, sems.at[0])]
    for z in range(ZS):
        cols = pl.ds(z // 2 * HD, HD)
        for n, source in enumerate((keys_ref, values_ref)):
            target = out_ref.at[z, pl.ds(n * TOK, TOK), :]
            copies.append(
                pltpu.make_async_copy(source.at[0, :, cols], target, sems.at[1 + 2 * z + n])
            )
    for copy in copies:
        copy.start()
    copies[0].wait()
    seg = seg_ref[...].astype(jnp.float32).astype(jnp.bfloat16)
    for z in range(ZS):
        out_ref[z, 2 * TOK : CHUNK, :] = jnp.broadcast_to(seg, (CHUNK - 2 * TOK, TOK))
    for copy in copies[1:]:
        copy.wait()


def keys_payload(keys, values, segments):
    return pl.pallas_call(
        keys_kernel,
        out_shape=jax.ShapeDtypeStruct((ZS, CHUNK, HD), jnp.bfloat16),
        in_specs=[HBM, HBM, HBM],
        out_specs=VMEM,
        scratch_shapes=[
            pltpu.VMEM((1, TOK), jnp.int32),
            pltpu.SemaphoreType.DMA((1 + 2 * ZS,)),
        ],
        compiler_params=params(),
        name="keys_payload",
    )(*in_hbm(keys, values, segments))


def rows_kernel(tasks_ref, queries_ref, go_ref, pk_ref, pv_ref, *rest):
    outs, sems = rest[: 3 * KVH], rest[3 * KVH]
    slot = tasks_ref[lax.axis_index("dp")] % 2
    zh = lax.axis_index("zh")
    half = PROMPT // 2
    copies = []

    def add(source, target):
        copies.append(pltpu.make_async_copy(source, target, sems.at[len(copies)]))

    for d in range(KVH):
        h = (zh + d) % KVH
        cols = pl.ds(pl.multiple_of(h * WIDE, WIDE), WIDE)
        q_out, go_out, prompt_out = outs[d], outs[KVH + d], outs[2 * KVH + d]
        add(queries_ref.at[0, :, cols], q_out)
        own = pl.ds(pl.multiple_of(h * HD, HD), HD)
        for n, bank in enumerate((pk_ref, pv_ref)):
            for s in range(2):
                place = pl.ds((2 * n + s) * HD, HD)
                add(
                    bank.at[slot, pl.ds(s * half, half), own],
                    prompt_out.at[:, place],
                )
        add(go_ref.at[0, :, cols], go_out)
    for copy in copies:
        copy.start()
    for copy in copies:
        copy.wait()


def rows_payload(tasks, queries, go, prompt_keys, prompt_values):
    outs = pl.pallas_call(
        rows_kernel,
        out_shape=[jax.ShapeDtypeStruct((TOK, WIDE), jnp.bfloat16)] * (2 * KVH)
        + [jax.ShapeDtypeStruct((PROMPT // 2, WIDE), jnp.bfloat16)] * KVH,
        in_specs=[SMEM, HBM, HBM, HBM, HBM],
        out_specs=[VMEM] * (3 * KVH),
        scratch_shapes=[pltpu.SemaphoreType.DMA((6 * KVH,))],
        compiler_params=params(),
        name="rows_payload",
    )(tasks, *in_hbm(queries, go, prompt_keys, prompt_values))
    return outs[:KVH], outs[KVH : 2 * KVH], outs[2 * KVH :]


class Bundle:
    def __init__(self, ref):
        self.ref = ref

    def keys(self, z):
        return self.ref[z, 0:TOK, :]

    def values(self, z):
        return self.ref[z, TOK : 2 * TOK, :]

    def segments(self, z):
        return self.ref[z, 2 * TOK : CHUNK, :].astype(jnp.float32)[0:1]


def accumulate(scores, wide, acc_ref, peak_ref, rows):
    old = peak_ref[rows]
    peak = jnp.maximum(old, jnp.max(scores, axis=1, keepdims=True))
    weights = jnp.exp2((scores - peak) * FACTOR).astype(jnp.bfloat16)
    shrink = jnp.exp2((old - peak) * FACTOR)
    acc_ref[rows] = acc_ref[rows] * shrink + dot_nn(weights, wide)
    peak_ref[rows] = peak


def absorb(bundles, j, q, seg_q, diagonal, acc_ref, peak_ref):
    zl, x, y = (lax.axis_index(name) for name in ("zl", "x", "y"))
    count = len(bundles) * 2 * TOK
    keys, values, visible = [], [], []
    for e in range(2):
        z = 2 * j + e
        for n, part in bundles.items():
            keys.append(part.keys(z))
            values.append(part.values(z))
            seg = part.segments(z)
            if diagonal and n != 0:
                b, c = ORDER[n]
                before = ((x + c + 4) % 4 * 2 + (y + b) % 2) < x * 2 + y
                shown = (zl > e) | ((zl == e) & before)
                seg = jnp.where(shown, seg, -1.0)
            same = seg_q == seg
            if diagonal and n == 0:
                reach = jnp.where(zl == e, 0, jnp.where(zl > e, TOK, -TOK))
                rows = lax.broadcasted_iota(jnp.int32, (TOK, TOK), 0)
                cols = lax.broadcasted_iota(jnp.int32, (TOK, TOK), 1)
                same = same & (cols - rows <= reach)
            visible.append(same)
    keys = jnp.concatenate(keys, axis=0)
    values = jnp.concatenate(values, axis=0)
    visible = jnp.concatenate(visible, axis=1)[None]
    wide = jnp.concatenate([values, jnp.ones(values.shape, jnp.bfloat16)], axis=1)
    size = GROUP * TOK // SPLIT
    scores = []
    for g in range(SPLIT):
        part = dot_nt(q[g * size : (g + 1) * size], keys).reshape(size // TOK, TOK, count)
        scores.append(jnp.where(visible, part, HIDDEN).reshape(size, count))
    for g in range(SPLIT):
        rows = slice(g * size, (g + 1) * size)
        accumulate(scores[g], wide, acc_ref, peak_ref, rows)


def sweep(bundles, own_ref, q, k, acc_ref, peak_ref):
    seg = own_ref[2 * k + lax.axis_index("zl"), 2 * TOK :, :].astype(jnp.float32)[0:1]
    seg_q = jnp.transpose(jnp.broadcast_to(seg, (TOK, TOK)))
    absorb(bundles, k, q, seg_q, True, acc_ref, peak_ref)

    def earlier(j, carry):
        absorb(bundles, j, q, seg_q, False, acc_ref, peak_ref)
        return carry

    lax.fori_loop(0, k, earlier, 0)


def first_kernel(names, *refs):
    q_refs, refs = refs[:KVH], refs[KVH:]
    bundles = {n: Bundle(ref) for n, ref in zip(names, refs)}
    refs = refs[len(names) :]
    out_ref, q_ref, state_ref, acc_ref, peak_ref, sems = refs
    own_ref = bundles[0].ref
    zh = lax.axis_index("zh")
    for d in range(KVH):
        q_ref[d] = stacked_heads(q_refs[d][...])

    def saved(d):
        return pltpu.make_async_copy(state_ref.at[d], out_ref.at[d], sems.at[d])

    def per_block(d, carry):
        acc_ref[...] = jnp.zeros_like(acc_ref)
        peak_ref[...] = jnp.full_like(peak_ref, HIDDEN)
        sweep(bundles, own_ref, q_ref[d], (zh - d + KVH) % KVH, acc_ref, peak_ref)
        state_ref[d, :, :HD] = acc_ref[:, :HD]
        lanes = lax.broadcasted_iota(jnp.int32, (GROUP * TOK, HD), 1)
        state_ref[d, :, HD:] = jnp.where(lanes < HD // 2, acc_ref[:, HD:], peak_ref[...])
        saved(d).start()
        return carry

    lax.fori_loop(0, KVH, per_block, 0)
    for d in range(KVH):
        saved(d).wait()


STATE = (KVH, GROUP * TOK, 2 * HD)


def cost(count):
    work = GROUP * TOK * HD * 4 * count * 2 * TOK * 10
    return pl.CostEstimate(flops=work, transcendentals=work // 512, bytes_accessed=1 << 22)


def attend_first(names, q, arrays):
    return pl.pallas_call(
        lambda *refs: first_kernel(names, *refs),
        out_shape=jax.ShapeDtypeStruct(STATE, jnp.float32),
        in_specs=[VMEM] * (KVH + len(arrays)),
        out_specs=pl.BlockSpec(memory_space=pltpu.HBM),
        scratch_shapes=[
            pltpu.VMEM((KVH, GROUP * TOK, HD), jnp.bfloat16),
            pltpu.VMEM(STATE, jnp.float32),
            pltpu.VMEM((GROUP * TOK, 2 * HD), jnp.float32),
            pltpu.VMEM((GROUP * TOK, 1), jnp.float32),
            pltpu.SemaphoreType.DMA((KVH,)),
        ],
        compiler_params=params(),
        cost_estimate=cost(len(names)),
        name="attend_first",
    )(*q, *arrays)


def last_kernel(names, *refs):
    q_refs, go_refs, refs = refs[:KVH], refs[KVH : 2 * KVH], refs[2 * KVH :]
    in_ref, own_ref, prompt_ref, *refs = refs
    bundles = {n: Bundle(ref) for n, ref in zip(names, refs)}
    refs = refs[len(names) :]
    att_refs, refs = refs[:KVH], refs[KVH:]
    grads_ref, q_ref, go_ref, state_ref, acc_ref, peak_ref, scores_ref, sems = refs
    zh = lax.axis_index("zh")

    def loaded(d):
        return pltpu.make_async_copy(in_ref.at[d], state_ref.at[d], sems.at[d])

    for d in range(KVH):
        loaded(d).start()
    for d in range(KVH):
        q_ref[d] = stacked_heads(q_refs[d][...])
        go_ref[d] = stacked_heads(go_refs[d][...])
    prompt_k = jnp.concatenate([prompt_ref[:, 0:HD], prompt_ref[:, HD : 2 * HD]], axis=0)
    prompt_v = jnp.concatenate([prompt_ref[:, 2 * HD : 3 * HD], prompt_ref[:, 3 * HD :]], axis=0)
    ones = jnp.ones(prompt_v.shape, jnp.bfloat16)
    prompt_wide = jnp.concatenate([prompt_v, ones], axis=1)

    blocks = range(KVH)
    for d in blocks:
        scores_ref[d] = dot_nt(q_ref[d], prompt_k)
    for d in blocks:
        loaded(d).wait()
    for d in blocks:
        acc_ref[d, :, :HD] = state_ref[d, :, :HD]
        acc_ref[d, :, HD:] = jnp.broadcast_to(state_ref[d, :, HD : HD + 1], (GROUP * TOK, HD))
        peak_ref[d] = state_ref[d, :, 2 * HD - 1 :]
    for d in blocks:
        accumulate(scores_ref[d], prompt_wide, acc_ref.at[d], peak_ref.at[d], slice(None))

    def per_block(d, carry):
        k = (zh - d + KVH) % KVH
        sweep(bundles, own_ref, q_ref[d], k, acc_ref.at[d], peak_ref.at[d])
        return carry

    lax.fori_loop(0, KVH, per_block, 0)
    lows, probs_lows = [], []
    for d in blocks:
        norm = acc_ref[d, :, HD:]
        attended = (acc_ref[d, :, :HD] / norm).astype(jnp.bfloat16)
        for g in range(GROUP):
            att_refs[d][:, g * HD : (g + 1) * HD] = attended[g * TOK : (g + 1) * TOK]
        go = go_ref[d]
        delta = jnp.sum(
            go.astype(jnp.float32) * attended.astype(jnp.float32), axis=1, keepdims=True
        )
        log_norm = peak_ref[d] * FACTOR + jnp.log2(norm)
        probs = jnp.exp2(scores_ref[d] * FACTOR - log_norm)
        score_grad = probs * (dot_nt(go, prompt_v) - delta)
        lows.append(score_grad.astype(jnp.bfloat16))
        probs_lows.append(probs.astype(jnp.bfloat16))
    everything = (KVH * GROUP * TOK, HD)
    key_part = dot_tn(jnp.concatenate(lows, axis=0), q_ref[...].reshape(everything)) * SCALE
    value_part = dot_tn(jnp.concatenate(probs_lows, axis=0), go_ref[...].reshape(everything))
    grads_ref[0:PROMPT, :] = key_part.astype(jnp.bfloat16)
    grads_ref[PROMPT:, :] = value_part.astype(jnp.bfloat16)


def attend_last(names, q, go, state, own, prompt, arrays):
    outs = pl.pallas_call(
        lambda *refs: last_kernel(names, *refs),
        out_shape=[jax.ShapeDtypeStruct((TOK, WIDE), jnp.bfloat16)] * KVH
        + [jax.ShapeDtypeStruct((2 * PROMPT, HD), jnp.bfloat16)],
        in_specs=[VMEM] * (2 * KVH)
        + [pl.BlockSpec(memory_space=pltpu.HBM)]
        + [VMEM] * (2 + len(arrays)),
        out_specs=[VMEM] * (KVH + 1),
        scratch_shapes=[
            pltpu.VMEM((KVH, GROUP * TOK, HD), jnp.bfloat16),
            pltpu.VMEM((KVH, GROUP * TOK, HD), jnp.bfloat16),
            pltpu.VMEM(STATE, jnp.float32),
            pltpu.VMEM((KVH, GROUP * TOK, 2 * HD), jnp.float32),
            pltpu.VMEM((KVH, GROUP * TOK, 1), jnp.float32),
            pltpu.VMEM((KVH, GROUP * TOK, HD), jnp.float32),
            pltpu.SemaphoreType.DMA((KVH,)),
        ],
        compiler_params=params(),
        cost_estimate=cost(len(names) + 1),
        name="attend_last",
    )(*q, *go, state, own, prompt, *arrays)
    return outs[:KVH], outs[KVH]


def sum_kernel(pieces_ref, out_ref):
    total = pieces_ref[0].astype(jnp.float32)
    for r in range(1, 8):
        total += pieces_ref[r].astype(jnp.float32)
    for r in range(8):
        out_ref[r] = total.astype(jnp.bfloat16)


def summed(pieces):
    return pl.pallas_call(
        sum_kernel,
        out_shape=jax.ShapeDtypeStruct((8, 32, HD), jnp.bfloat16),
        in_specs=[VMEM],
        out_specs=VMEM,
        compiler_params=params(),
        name="summed",
    )(pieces)


def pairs_kernel(sent_ref, out_ref):
    for h in range(KVH):
        total = sent_ref[2 * h].astype(jnp.float32) + sent_ref[2 * h + 1].astype(jnp.float32)
        out_ref[h] = total.astype(jnp.bfloat16)


def pairs_summed(sent):
    return pl.pallas_call(
        pairs_kernel,
        out_shape=jax.ShapeDtypeStruct((KVH, 32, HD), jnp.bfloat16),
        in_specs=[VMEM],
        out_specs=VMEM,
        compiler_params=params(),
        name="pairs_summed",
    )(sent)


def route_kernel(tasks_ref, *refs):
    parts, out_ref = refs[:4], refs[4]
    dp = lax.axis_index("dp")
    first = (lax.axis_index("zh") * 2 + lax.axis_index("zl")) * 16
    places = [tasks_ref[dp ^ d] - first for d in range(4)]
    here = [(place >= 0) & (place < 16) for place in places]
    out_ref[...] = jnp.zeros_like(out_ref)
    for d in range(4):

        @pl.when(here[d])
        def _():
            total = parts[d][...].astype(jnp.float32)
            for e in range(d):
                same = here[e] & (places[e] == places[d])
                total += jnp.where(same, parts[e][...].astype(jnp.float32), 0.0)
            out_ref[jnp.clip(places[d], 0, 15)] = total.astype(jnp.bfloat16)


def route(tasks, parts):
    return pl.pallas_call(
        route_kernel,
        out_shape=jax.ShapeDtypeStruct((16, KVH, 32, HD), jnp.bfloat16),
        in_specs=[SMEM] + [VMEM] * 4,
        out_specs=VMEM,
        compiler_params=params(),
        name="route",
    )(tasks, *parts)


def banks_kernel(banks_ref, key_ref, value_ref):
    for r in range(8):
        out_ref = key_ref if r < 4 else value_ref
        rows = slice(r % 4 * 32, r % 4 * 32 + 32)
        for j in range(2):
            for h in range(KVH):
                part = banks_ref[2 * r + j, h].astype(jnp.float32)
                out_ref[j, rows, h * HD : (h + 1) * HD] = part


def banks_out(banks):
    shape = jax.ShapeDtypeStruct((2, PROMPT, KVH * HD), jnp.float32)
    return pl.pallas_call(
        banks_kernel,
        out_shape=(shape, shape),
        compiler_params=params(),
        name="banks_out",
    )(banks)


def heads_kernel(*refs):
    out_ref = refs[KVH]
    zh = lax.axis_index("zh")
    for d in range(KVH):
        h = (zh + d) % KVH
        out_ref[0, :, pl.ds(pl.multiple_of(h * WIDE, WIDE), WIDE)] = refs[d][...]


def heads_out(parts):
    return pl.pallas_call(
        heads_kernel,
        out_shape=jax.ShapeDtypeStruct((1, TOK, KVH * WIDE), jnp.bfloat16),
        compiler_params=params(),
        name="heads_out",
    )(*parts)


def swap(value, axis):
    return lax.ppermute(value, axis, [(0, 1), (1, 0)])


def from_left(value):
    return lax.ppermute(value, "x", [(i, (i + 1) % 4) for i in range(4)])


def from_right(value):
    return lax.ppermute(value, "x", [(i, (i - 1) % 4) for i in range(4)])


def crosswise(value, step):
    pairs = [(x * 2 + y, (x + step) % 4 * 2 + 1 - y) for x in range(4) for y in range(2)]
    return lax.ppermute(value, ("x", "y"), pairs)


def turned(parts, sign):
    moved = [parts[0]]
    for d in range(1, KVH):
        moved.append(
            lax.ppermute(parts[d], "zh", [(i, (i + sign * d) % 4) for i in range(4)])
        )
    return moved


def exchange(blocks, axes):
    return lax.all_to_all(blocks, axes, 0, 0, tiled=True)


def choose_kernel(stage, tasks_ref, *refs):
    parts, out_ref = refs[:-1], refs[-1]
    owner = tasks_ref[lax.axis_index("dp")] // 2
    if stage == "zh":
        wanted = (lax.axis_index("zh") + KVH - owner // 16) % KVH
    elif stage == "zl":
        wanted = (owner // 8 + lax.axis_index("zl")) % 2
    elif stage == "y":
        wanted = (owner + lax.axis_index("y")) % 2
    else:
        wanted = (lax.axis_index("x") + 4 - (owner // 2) % 4) % 4
    for n in range(len(parts)):

        @pl.when(wanted == n)
        def _():
            out_ref[...] = parts[n][...]


def choose(stage, tasks, parts):
    return pl.pallas_call(
        lambda *refs: choose_kernel(stage, *refs),
        out_shape=jax.ShapeDtypeStruct(parts[0].shape, parts[0].dtype),
        in_specs=[SMEM] + [VMEM] * len(parts),
        out_specs=VMEM,
        compiler_params=params(4),
    )(tasks, *parts)


def in_hbm(*arrays):
    return [pltpu.with_memory_space_constraint(array, pltpu.HBM) for array in arrays]


def step(queries, keys, values, segments, task_ids, prompt_keys, prompt_values, grad_out):
    payload = keys_payload(keys, values, segments)
    own = exchange(payload, ("zh", "zl"))
    q, go, prompts = rows_payload(
        task_ids, queries, grad_out, prompt_keys, prompt_values
    )
    prompts = turned(prompts, 1)

    beside = swap(own, "y")
    left = from_left(own)
    right = from_right(own)
    q = turned(q, 1)
    across = from_left(left)
    beside_across = crosswise(right, -1)
    beside_left = from_left(beside)
    beside_right = from_right(beside)
    go = turned(go, 1)

    prompt = choose("zh", task_ids, prompts)
    flipped = swap(prompt, "zl")
    prompt = choose("zl", task_ids, (prompt, flipped))
    beyond = swap(prompt, "y")
    prompt = choose("y", task_ids, (prompt, beyond))
    far = lax.ppermute(prompt, "x", [(i, (i + 2) % 4) for i in range(4)])
    prompt_left = from_left(prompt)
    prompt_right = from_right(prompt)
    prompt = choose("x", task_ids, (prompt, prompt_left, far, prompt_right))

    state = attend_first((0, 1, 2, 3), q, (own, beside, left, right))
    attended, grads = attend_last(
        (4, 5, 6, 7),
        q,
        go,
        state,
        own,
        prompt,
        (across, beside_left, beside_right, beside_across),
    )

    attended = turned(attended, -1)
    pieces = exchange(grads.reshape(8, 32, HD), ("x", "y"))
    sent = exchange(summed(pieces), ("zh", "zl"))
    mine = pairs_summed(sent)
    parts = [mine]
    for d in range(1, 4):
        parts.append(lax.ppermute(mine, "dp", [(i, i ^ d) for i in range(4)]))
    routed = route(task_ids, parts)
    banks = exchange(routed, ("x", "y"))
    key_grad, value_grad = banks_out(banks)
    return heads_out(attended), key_grad, value_grad


def solution(mesh):
    split = Mesh(mesh.devices.reshape(4, 4, 2, 4, 2), ALL)
    return jax.shard_map(
        step,
        mesh=split,
        in_specs=(
            P("dp", SEQ, None),
            P("dp", SEQ, None),
            P("dp", SEQ, None),
            P("dp", SEQ),
            P(),
            P(SEQ, None, None),
            P(SEQ, None, None),
            P("dp", SEQ, None),
        ),
        out_specs=(P("dp", SEQ, None), P(SEQ, None, None), P(SEQ, None, None)),
        check_vma=False,
    )
```
